32 devices in a mesh: dp: 4 (over z), row: 8 (over y, x, core).
Axes of the slice: x: 2, y: 2, z: 4, core: 2. Of those that a mesh axis runs over, the one named last changes fastest.
Arguments:
- fields: bfloat16 [4, 16, 512, 2048], P('dp', None, 'row'), may hold values from -6 to 6
- cotangent: bfloat16 [4, 16, 512, 2048], P('dp', None, 'row'), may hold values from -6 to 6
- spectral: bfloat16 [2, 16, 16, 128, 128], P(None, None, None, 'row'), may hold values from -5 to 5
- local_weight: bfloat16 [16, 16], replicated, may hold values from -1.5 to 1.5
- bias: float32 [16], replicated, may hold values from -3 to 3
Outputs:
- field_grad: bfloat16 [4, 16, 512, 2048], P('dp', None, 'row')
- spectral_grad: float32 [2, 16, 16, 128, 128], P(None, None, 'dp', 'row')
- local_grad: float32 [16, 16], replicated
- bias_grad: float32 [16], replicated
The draws below stay inside these ranges and needn't reach their ends.
All inputs are finite; a program needn't handle non-finite values.
Results may differ from the reference program's by a relative error of at most 0.028.
Values may be sent and summed in bfloat16 or wider, within the bound.
No kernel may reach another device: no remote copies, remote signals or barrier semaphores. Data moves between devices by JAX's collectives and lax.ppermute only.
A program may use at most 128 MiB of HBM per device.

```python
import math
import jax
import jax.numpy as jnp
from jax import lax

C = 16
W = 2048
M = 128
H = 512
NMAP = 4


def spiked(result, key, source, target, blocks, factor):
    owner, partner = [(jnp.arange(result.shape[position]) // (result.shape[position] // blocks)).reshape([-1 if axis == position else 1 for axis in range(result.ndim)]) for position in (source, target)]
    chosen = jax.random.permutation(key, blocks)[partner]
    strong = (owner == chosen) | (owner == (partner + blocks // 2) % blocks)
    return jnp.where(strong, factor * result, result)


def block_levels(key, shape, pieces, low, largest):
    def one(position, shards_of):
        steps = jax.random.uniform(jax.random.fold_in(jax.random.fold_in(key, 6), position), (shards_of,), jnp.float32, low / len(pieces), largest / len(pieces))
        return jnp.repeat(jnp.exp(steps), shape[position] // shards_of).reshape((-1,) + (1,) * (len(shape) - position - 1))

    gain = one(*pieces[0])
    for cut in pieces[1:]:
        gain = gain * one(*cut)
    return gain


def scatter_about(key, extent, scale, limit, pieces=(), kind=jnp.bfloat16):
    array = scale * jax.random.normal(key, extent, jnp.float32)
    if pieces:
        array = array * block_levels(key, extent, pieces, -0.22, 0.18)
    return jnp.clip(array, -limit, limit).astype(kind)


def gaussian_with(own_key, dims, scale, most, pieces, heavy, kind=jnp.bfloat16):
    drawn = scale * jax.random.normal(own_key, dims, jnp.float32)
    if pieces:
        drawn = drawn * block_levels(own_key, dims, pieces, -0.22, 0.18)
    return jnp.clip(spiked(drawn, jax.random.fold_in(own_key, 3), *heavy), -most, most).astype(kind)


def setup_inputs(seed: int = 0) -> dict:
    keys = jax.random.split(jax.random.key(seed), 6)
    fields = scatter_about(keys[0], (NMAP, C, H, W), 1.0, 6.0, ((0, 4), (2, 8)))
    cotangent = gaussian_with(keys[1], (NMAP, C, H, W), 1.0, 6.0, ((0, 4), (2, 8)), (0, 1, 4, 2.0))
    spectral = scatter_about(keys[2], (2, C, C, M, M), 1.0, 5.0, ((3, 8),))
    local_weight = scatter_about(keys[3], (C, C), C ** -0.5, 1.5)
    bias = scatter_about(keys[4], (C,), 0.5, 3.0, (), jnp.float32)
    return dict(fields=fields, cotangent=cotangent, spectral=spectral, local_weight=local_weight, bias=bias)


def phase_angle(freq, pos, count):
    turns = freq[:, None] % count * pos[None, :] % count
    return 2.0 * math.pi / count * turns.astype(jnp.float32)

def row_phases(first, length, height, modes):
    freq = jnp.arange(modes, dtype=jnp.int32) - modes // 2
    place = first + jnp.arange(length, dtype=jnp.int32)
    angle = phase_angle(freq, place, height)
    return jnp.stack([jnp.cos(angle), jnp.sin(angle)], axis=0).astype(jnp.bfloat16)

def column_forward(width, modes):
    angle = phase_angle(jnp.arange(modes, dtype=jnp.int32), jnp.arange(width, dtype=jnp.int32), width).T
    table = jnp.stack([jnp.cos(angle), -jnp.sin(angle)], axis=1)
    return table.reshape(width, 2 * modes).astype(jnp.bfloat16)

def column_inverse(width, modes, double):
    angle = phase_angle(jnp.arange(modes, dtype=jnp.int32), jnp.arange(width, dtype=jnp.int32), width)
    weight = jnp.where(jnp.arange(modes) == 0, 1.0, 2.0 if double else 1.0).astype(jnp.float32)[:, None]
    table = jnp.stack([weight * jnp.cos(angle), -weight * jnp.sin(angle)], axis=0)
    return table.reshape(2 * modes, width).astype(jnp.bfloat16)

def row_forward(phases, spectrum):
    parts = jnp.einsum('tah,chrb->tacrb', phases.astype(jnp.float32), spectrum.astype(jnp.float32))
    real = parts[0, :, :, 0] + parts[1, :, :, 1]
    imag = parts[0, :, :, 1] - parts[1, :, :, 0]
    return jnp.stack([real, imag], axis=2)

def row_inverse(phases, modes_in):
    parts = jnp.einsum('tah,aorb->tohrb', phases.astype(jnp.float32), modes_in.astype(jnp.float32))
    real = parts[0, :, :, 0] - parts[1, :, :, 1]
    imag = parts[0, :, :, 1] + parts[1, :, :, 0]
    return jnp.stack([real, imag], axis=2)

def product(left, right):
    return jnp.einsum('coab,acb->aob', left, right, precision=lax.Precision.HIGHEST)

def mix_modes(weights, spectrum):
    real = product(weights[0], spectrum[:, :, 0]) - product(weights[1], spectrum[:, :, 1])
    imag = product(weights[0], spectrum[:, :, 1]) + product(weights[1], spectrum[:, :, 0])
    return jnp.stack([real, imag], axis=2)

def outer(left, right):
    return jnp.einsum('aob,acb->coab', left, right, precision=lax.Precision.HIGHEST)

def back_product(weight, grad):
    return jnp.einsum('coab,aob->acb', weight, grad, precision=lax.Precision.HIGHEST)

def weight_terms(grad_modes, spectrum):
    real = outer(grad_modes[:, :, 0], spectrum[:, :, 0]) + outer(grad_modes[:, :, 1], spectrum[:, :, 1])
    imag = outer(grad_modes[:, :, 1], spectrum[:, :, 0]) - outer(grad_modes[:, :, 0], spectrum[:, :, 1])
    return jnp.stack([real, imag], axis=0)

def adjoint_modes(weights, grad_modes):
    real = back_product(weights[0], grad_modes[:, :, 0]) + back_product(weights[1], grad_modes[:, :, 1])
    imag = back_product(weights[0], grad_modes[:, :, 1]) - back_product(weights[1], grad_modes[:, :, 0])
    return jnp.stack([real, imag], axis=2)

def reference(fields, cotangent, spectral, local_weight, bias):
    norm_scale = 1.0 / math.sqrt(H * W)
    grad_scale = 1.0 / math.sqrt(NMAP * H * W)
    phases = row_phases(0, H, H, M)
    forward_cols = column_forward(W, M)
    inverse_double = column_inverse(W, M, True)
    inverse_single = column_inverse(W, M, False)
    doubling = jnp.where(jnp.arange(M) == 0, 1.0, 2.0).astype(jnp.float32)
    weights = spectral.astype(jnp.float32)
    local_float = local_weight.astype(jnp.float32)

    def one_map(pair):
        field, cot = pair
        coeffs = jnp.dot(field.reshape(C * H, W), forward_cols, preferred_element_type=jnp.float32)
        coeffs = coeffs.astype(jnp.bfloat16).reshape(C, H, 2, M)
        spectrum = norm_scale * row_forward(phases, coeffs)
        mixed = mix_modes(weights, spectrum).astype(jnp.bfloat16)
        back_rows = row_inverse(phases, mixed).astype(jnp.bfloat16)
        spec_out = norm_scale * jnp.dot(back_rows.reshape(C * H, 2 * M), inverse_double, preferred_element_type=jnp.float32).reshape(C, H, W)
        preact = spec_out + jnp.einsum('co,chw->ohw', local_float, field.astype(jnp.float32)) + bias[:, None, None]
        unused, pull = jax.vjp(jax.nn.gelu, preact)
        grad_pre = pull(cot.astype(jnp.float32))[0].astype(jnp.bfloat16)
        grad_coeffs = jnp.dot(grad_pre.reshape(C * H, W), forward_cols, preferred_element_type=jnp.float32)
        grad_coeffs = grad_coeffs.astype(jnp.bfloat16).reshape(C, H, 2, M)
        grad_modes = norm_scale * row_forward(phases, grad_coeffs) * doubling
        weight_term = weight_terms(grad_modes, spectrum)
        freq_grad = adjoint_modes(weights, grad_modes).astype(jnp.bfloat16)
        grad_rows = row_inverse(phases, freq_grad).astype(jnp.bfloat16)
        field_grad = norm_scale * jnp.dot(grad_rows.reshape(C * H, 2 * M), inverse_single, preferred_element_type=jnp.float32).reshape(C, H, W)
        field_grad = field_grad + jnp.einsum('co,ohw->chw', local_float, grad_pre.astype(jnp.float32))
        local_term = grad_scale * jnp.einsum('chw,ohw->co', field.astype(jnp.float32), grad_pre.astype(jnp.float32))
        bias_term = grad_scale * lax.optimization_barrier(jnp.sum(grad_pre.astype(jnp.float32), axis=(1, 2)))
        return (field_grad.astype(jnp.bfloat16), weight_term, local_term, bias_term)
    field_grad, weight_term, local_term, bias_term = lax.map(one_map, (fields, cotangent))
    return (field_grad, lax.optimization_barrier(jnp.sum(weight_term, axis=0)), lax.optimization_barrier(jnp.sum(local_term, axis=0)), lax.optimization_barrier(jnp.sum(bias_term, axis=0)))
```

```python
import functools
import math

import jax
import jax.numpy as jnp
import numpy as np
from jax import lax
from jax.experimental import pallas as pl
from jax.experimental.pallas import tpu as pltpu
from jax.sharding import PartitionSpec as P


BF16 = jnp.bfloat16
F32 = jnp.float32
LANES = 128
GROUP = 16


def column_table(width, modes):
    turns = np.arange(modes)[:, None] * np.arange(width)[None, :] % width
    angle = np.float32(2.0 * math.pi / width) * turns.astype(np.float32)
    table = np.concatenate([np.cos(angle), -np.sin(angle)], axis=0)
    return table.astype(BF16)


def row_angles(mode, place, height, modes):
    freq = (mode - modes // 2) % height
    turns = freq[:, None] * place[None, :] % height
    return 2.0 * math.pi / height * turns.astype(F32)


def dot(left, right):
    return jnp.dot(left, right, preferred_element_type=F32)


def dot_nt(left, right):
    return lax.dot_general(left, right, (((1,), (1,)), ((), ())), preferred_element_type=F32)


def tree(parts):
    parts = list(parts)
    while len(parts) > 1:
        parts = [parts[at] + parts[at + 1] for at in range(0, len(parts), 2)]
    return parts[0]


def whole(shape):
    return pl.BlockSpec(shape, lambda *_: (0,) * len(shape))


def call(kernel, name, out_shape, in_shapes, flops, **more):
    return pl.pallas_call(
        kernel,
        name=name,
        out_shape=out_shape,
        cost_estimate=pl.CostEstimate(flops=flops, transcendentals=0, bytes_accessed=1 << 20),
        **more,
    )


def to_pieces(value):
    first = value.astype(BF16).astype(F32)
    rest = value - first
    second = rest.astype(BF16).astype(F32)
    third = rest - second
    return first + pltpu.roll(second, 32, 1) + pltpu.roll(third, 64, 1)


def from_pieces(packed):
    back = LANES
    return packed + pltpu.roll(packed, back - 32, 1) + pltpu.roll(packed, back - 64, 1)


def columns_kernel(chans, field_ref, table_ref, out_ref):
    width = field_ref.shape[2]
    lanes = table_ref.shape[1]
    sums = dot(field_ref[...].reshape(chans * GROUP, width), table_ref[...]).astype(BF16)
    for c in range(chans):
        out_ref[:, c * lanes : (c + 1) * lanes] = sums[c * GROUP : (c + 1) * GROUP]


def rows_kernel(chans, modes, scale, extra, mine_ref, other_ref, phase_ref, *outs):
    half = phase_ref.shape[0] // 2
    lanes = 2 * modes
    phase = phase_ref[...]
    for c in range(chans):
        at = slice(c * lanes, (c + 1) * lanes)
        both = jnp.concatenate([mine_ref[:, at], other_ref[:, at]], axis=0)
        part = dot(phase, both)
        real = part[:half, :modes] + part[half:, modes:]
        imag = part[:half, modes:] - part[half:, :modes]
        full = (scale * jnp.concatenate([real, imag], axis=1)).astype(BF16)
        size = half // len(outs)
        for d, out in enumerate(outs):
            out[:, at] = full[d * size : (d + 1) * size]
    if extra:
        top = chans * lanes
        rows = chans
        total = from_pieces(mine_ref[:rows, top:].astype(F32)) + from_pieces(
            other_ref[:rows, top:].astype(F32)
        )
        packed = to_pieces(keep_low(total)).astype(BF16)
        for out in outs:
            for d in range(len(outs) if len(outs) == 1 else 1):
                put_pieces(out, packed, top, rows)


def keep_low(value):
    lane = lax.broadcasted_iota(jnp.int32, value.shape, 1)
    return jnp.where(lane < 32, value, 0.0)


def put_pieces(out, packed, top, rows):
    size = out.shape[0]
    if size >= rows:
        out[:rows, top : top + LANES] = packed
        if size > rows:
            out[rows:, top : top + LANES] = jnp.zeros((size - rows, LANES), packed.dtype)
        return
    for e in range(rows // size):
        out[:, top + e * LANES : top + (e + 1) * LANES] = packed[e * size : (e + 1) * size]


def get_pieces(ref, top, rows):
    size = ref.shape[0]
    if size >= rows:
        return ref[:rows, top : top + LANES].astype(F32)
    return jnp.concatenate(
        [
            ref[:, top + e * LANES : top + (e + 1) * LANES].astype(F32)
            for e in range(rows // size)
        ],
        axis=0,
    )


def mix_kernel(chans, modes, count, weight_ref, *refs):
    chunks = refs[:count]
    mixed_ref, spectrum_ref, sums = refs[count:]
    lanes = 2 * modes
    for c in range(2 * chans):
        at = slice(c * modes, (c + 1) * modes)
        value = tree([chunk[:, at].astype(F32) for chunk in chunks])
        sums[c] = value
        spectrum_ref[:, at] = value.astype(BF16)

    for o in range(chans):
        real = imag = None
        for c in range(chans):
            wr = weight_ref[0, c, o].astype(F32)
            wi = weight_ref[1, c, o].astype(F32)
            fr = sums[2 * c]
            fi = sums[2 * c + 1]
            a = wr * fr - wi * fi
            b = wr * fi + wi * fr
            real = a if real is None else real + a
            imag = b if imag is None else imag + b
        mixed_ref[:, o * lanes : o * lanes + modes] = real.astype(BF16)
        mixed_ref[:, o * lanes + modes : (o + 1) * lanes] = imag.astype(BF16)


def back_kernel(chans, modes, count, maps, where_ref, weight_ref, *refs):
    chunks = refs[:count]
    back_ref = refs[count]
    slices = refs[count + 1 : count + 1 + maps]
    sums, gathered = refs[count + 1 + maps :]
    lanes = 2 * modes
    shape = (chunks[0].shape[0], modes)
    doubling = jnp.where(lax.broadcasted_iota(jnp.int32, shape, 1) == 0, 1.0, 2.0)
    for c in range(2 * chans):
        at = slice(c * modes, (c + 1) * modes)
        value = tree([chunk[:, at].astype(F32) for chunk in chunks]) * doubling
        sums[c] = value
        gathered[:, at] = value.astype(BF16)

    for c in range(chans):
        real = imag = None
        for o in range(chans):
            wr = weight_ref[0, c, o].astype(F32)
            wi = weight_ref[1, c, o].astype(F32)
            gr = sums[2 * o]
            gi = sums[2 * o + 1]
            a = wr * gr + wi * gi
            b = wr * gi - wi * gr
            real = a if real is None else real + a
            imag = b if imag is None else imag + b
        back_ref[:, c * lanes : c * lanes + modes] = real.astype(BF16)
        back_ref[:, c * lanes + modes : (c + 1) * lanes] = imag.astype(BF16)

    top = chans * lanes
    total = tree([from_pieces(get_pieces(chunk, top, chans)) for chunk in chunks])
    packed = to_pieces(keep_low(total)).astype(BF16)
    span = chans // maps * lanes
    for d, out in enumerate(slices):
        first = pl.multiple_of((where_ref[0] ^ d) * span, LANES)
        out[:, :span] = gathered[:, pl.ds(first, span)]
        put_pieces(out, packed, span, chans)


def weight_kernel(chans, modes, maps, scale, *refs):
    spectra = refs[:maps]
    slices = refs[maps : 2 * maps]
    grad_ref, small_ref = refs[2 * maps :]
    lanes = 2 * modes
    part = chans // maps
    for o in range(part):
        at = o * lanes
        grads = [
            (s[:, at : at + modes].astype(F32), s[:, at + modes : at + lanes].astype(F32))
            for s in slices
        ]
        for c in range(chans):
            at = c * lanes
            real = []
            imag = []
            for spectrum, (gr, gi) in zip(spectra, grads):
                fr = spectrum[:, at : at + modes].astype(F32)
                fi = spectrum[:, at + modes : at + lanes].astype(F32)
                real.append(gr * fr + gi * fi)
                imag.append(gi * fr - gr * fi)
            grad_ref[0, c, o] = tree(real)
            grad_ref[1, c, o] = tree(imag)
    small_ref[...] = scale * tree([from_pieces(get_pieces(s, part * lanes, chans)) for s in slices])


def channel_map(local_ref, chans, back):
    size = chans * GROUP
    pick = (
        lax.broadcasted_iota(jnp.int32, (size, chans), 0) // GROUP
        == lax.broadcasted_iota(jnp.int32, (size, chans), 1)
    )
    pick = jnp.where(pick, 1.0, 0.0).astype(BF16)
    local = local_ref[...]
    if back:
        wide = dot(pick, local).astype(BF16)
    else:
        wide = lax.dot_general(
            pick, local, (((1,), (1,)), ((), ())), preferred_element_type=F32
        ).astype(BF16)
    full = dot_nt(wide, pick)
    row = lax.broadcasted_iota(jnp.int32, (size, size), 0) % GROUP
    lane = lax.broadcasted_iota(jnp.int32, (size, size), 1) % GROUP
    return jnp.where(row == lane, full, 0.0).astype(BF16)


def inverse_rows(chans, modes, scale, phase, chunks, doubled, out):
    lanes = 2 * modes
    half = phase.shape[0] // 2
    factor = jnp.full((1, modes), scale, F32)
    if doubled:
        first = lax.broadcasted_iota(jnp.int32, (1, modes), 1) == 0
        factor = jnp.where(first, scale, 2.0 * scale)
    for o in range(chans):
        at = slice(o * lanes, (o + 1) * lanes)
        part = dot(phase, jnp.concatenate([chunk[:, at] for chunk in chunks], axis=0))
        real = ((part[:half, :modes] - part[half:, modes:]) * factor).astype(BF16)
        imag = ((part[:half, modes:] + part[half:, :modes]) * factor).astype(BF16)
        for block in range(half // GROUP):
            rows = slice(block * GROUP, (block + 1) * GROUP)
            place = slice(o * GROUP, (o + 1) * GROUP)
            out[block, place, :modes] = real[rows]
            out[block, place, modes:] = imag[rows]


SLOPE = math.sqrt(2.0 / math.pi)
CUBIC = 0.044715


def gelu_slope(x):
    square = x * x
    t = jnp.tanh(x * (SLOPE + (SLOPE * CUBIC) * square))
    rest = x * (0.5 * SLOPE + (1.5 * SLOPE * CUBIC) * square)
    return (0.5 + 0.5 * t) + (1.0 - t * t) * rest


def main_kernel(chans, modes, scale, tile, count, *refs):
    chunks = refs[:count]
    (phase_ref, inverse_ref, forward_ref, local_ref, bias_ref, field_ref, cot_ref) = refs[
        count : count + 7
    ]
    grad_ref, sums_ref, rows, mixer, local_sum, bias_sum = refs[count + 7 :]
    step = pl.program_id(0)
    size = chans * GROUP
    width = field_ref.shape[2]
    lanes = 2 * modes

    @pl.when(step == 0)
    def _():
        inverse_rows(chans, modes, scale, phase_ref[...], chunks, True, rows)
        mixer[...] = channel_map(local_ref, chans, False)
        local_sum[...] = jnp.zeros_like(local_sum)
        bias_sum[...] = jnp.zeros_like(bias_sum)
        sums_ref[...] = jnp.zeros_like(sums_ref)

    mine = rows[step]
    mix = mixer[...]
    group = lax.broadcasted_iota(jnp.int32, (size, chans), 0) // GROUP
    pick = group == lax.broadcasted_iota(jnp.int32, (size, chans), 1)
    bias = jnp.sum(jnp.where(pick, bias_ref[...], 0.0), axis=1, keepdims=True)
    total = jnp.zeros((size, lanes), F32)
    outer = jnp.zeros((size, size), F32)
    for at in range(0, width, tile):
        span = slice(at, at + tile)
        field = field_ref[:, :, span].reshape(size, tile)
        preact = dot(mix, field) + dot(mine, inverse_ref[:, span]) + bias
        cot = cot_ref[:, :, span].reshape(size, tile).astype(F32)
        grad = (cot * gelu_slope(preact)).astype(BF16)
        grad_ref[:, :, span] = grad.reshape(chans, GROUP, tile)
        total = total + dot(grad, forward_ref[span, :])
        outer = outer + dot_nt(field, grad)
    local_sum[...] += outer
    bias_sum[...] += total[:, :modes]
    here = pl.ds(pl.multiple_of(step * GROUP, GROUP), GROUP)
    rounded = total.astype(BF16)
    for o in range(chans):
        sums_ref[here, o * lanes : (o + 1) * lanes] = rounded[o * GROUP : (o + 1) * GROUP]

    @pl.when(step == pl.num_programs(0) - 1)
    def _():
        row = lax.broadcasted_iota(jnp.int32, (size, size), 0) % GROUP
        lane = lax.broadcasted_iota(jnp.int32, (size, size), 1) % GROUP
        same = jnp.where(row == lane, local_sum[...], 0.0).reshape(chans, GROUP, size)
        folded = jnp.sum(same, axis=1)
        wide = lax.broadcasted_iota(jnp.int32, (size, LANES), 0) // GROUP
        gather = wide == lax.broadcasted_iota(jnp.int32, (size, LANES), 1)
        local = jnp.dot(
            folded,
            jnp.where(gather, 1.0, 0.0),
            precision=lax.Precision.HIGHEST,
            preferred_element_type=F32,
        )
        biases = jnp.sum(bias_sum[...].reshape(chans, GROUP, modes), axis=1)[:, :1]
        place = lax.broadcasted_iota(jnp.int32, (chans, LANES), 1)
        small = jnp.where(place == chans, biases, jnp.where(place < chans, local, 0.0))
        sums_ref[:chans, chans * lanes :] = to_pieces(small).astype(BF16)


def field_kernel(chans, modes, scale, tile, count, *refs):
    chunks = refs[:count]
    phase_ref, inverse_ref, local_ref, grad_ref, out_ref, rows, mixer = refs[count:]
    step = pl.program_id(0)
    size = chans * GROUP
    width = grad_ref.shape[2]

    @pl.when(step == 0)
    def _():
        inverse_rows(chans, modes, scale, phase_ref[...], chunks, False, rows)
        mixer[...] = channel_map(local_ref, chans, True)

    mine = rows[step]
    mix = mixer[...]
    for at in range(0, width, tile):
        span = slice(at, at + tile)
        grad = grad_ref[:, :, span].reshape(size, tile)
        value = dot(mix, grad) + dot(mine, inverse_ref[:, span])
        out_ref[:, :, span] = value.astype(BF16).reshape(chans, GROUP, tile)


def swap(value, axis, mask):
    size = lax.axis_size(axis)
    return lax.ppermute(value, axis, [(at, at ^ mask) for at in range(size)])


def on_device(fields, cotangent, spectral, local_weight, bias):
    field = fields[0]
    cot = cotangent[0]
    chans, rows_here, width = field.shape
    owned, modes = spectral.shape[3:]
    row_count = lax.axis_size("row")
    map_count = lax.axis_size("dp")
    chips = row_count // 2
    height = rows_here * row_count
    scale = 1.0 / math.sqrt(height * width)
    grad_scale = 1.0 / math.sqrt(map_count * height * width)
    lanes = 2 * modes
    flat = chans * lanes
    size = chans * GROUP
    blocks = rows_here // GROUP
    extra = LANES * max(1, chans // owned)
    aligned = owned % GROUP == 0

    me = lax.axis_index("row")
    chip, core = me // 2, me % 2
    inverse_const = column_table(width, modes)
    inverse = jnp.asarray(inverse_const)
    forward = jnp.asarray(np.ascontiguousarray(inverse_const.T))

    near = jnp.arange(chips, dtype=jnp.int32) ^ chip
    inner = jnp.arange(owned, dtype=jnp.int32)
    own_modes = ((2 * near + core)[:, None] * owned + inner[None, :]).reshape(-1)
    far_modes = ((2 * near + 1 - core)[:, None] * owned + inner[None, :]).reshape(-1)
    here = jnp.arange(rows_here, dtype=jnp.int32)
    pair_rows = jnp.concatenate([me * rows_here + here, (me ^ 1) * rows_here + here])
    angle = row_angles(own_modes, pair_rows, height, modes)
    to_modes = jnp.concatenate([jnp.cos(angle), jnp.sin(angle)], axis=0).astype(BF16)
    all_modes = jnp.concatenate([own_modes, far_modes])
    angle = row_angles(all_modes, me * rows_here + here, height, modes).T
    to_rows = jnp.concatenate([jnp.cos(angle), jnp.sin(angle)], axis=0).astype(BF16)

    block = pl.BlockSpec((chans, GROUP, width), lambda i: (0, i, 0))

    def rows_step(mine, other, more):
        out_lanes = flat + (extra if more else 0)
        if aligned:
            shapes = [jax.ShapeDtypeStruct((owned, out_lanes), BF16)] * chips
        else:
            shapes = [jax.ShapeDtypeStruct((chips * owned, flat), BF16)]
        kernel = functools.partial(rows_kernel, chans, modes, scale, more and aligned)
        outs = pl.pallas_call(
            kernel,
            name="rows",
            out_shape=shapes,
            cost_estimate=pl.CostEstimate(
                flops=4 * chips * owned * 2 * rows_here * flat,
                transcendentals=0,
                bytes_accessed=6 * rows_here * flat,
            ),
        )(mine, other, to_modes)
        if aligned:
            return outs
        pieces = jnp.split(outs[0], chips, axis=0)
        if more:
            packed = small_sum(mine[:chans, flat:], other[:chans, flat:])
            packed = packed.reshape(chans // owned, owned, LANES).transpose(1, 0, 2)
            packed = packed.reshape(owned, extra)
            pieces = [jnp.concatenate([piece, packed], axis=1) for piece in pieces]
        return pieces

    def small_sum(mine, other):
        def kernel(a, b, out):
            total = from_pieces(a[...].astype(F32)) + from_pieces(b[...].astype(F32))
            out[...] = to_pieces(keep_low(total)).astype(BF16)

        return pl.pallas_call(
            kernel, name="small", out_shape=jax.ShapeDtypeStruct((chans, LANES), BF16)
        )(mine, other)

    def spread(pieces):
        return [pieces[0]] + [swap(pieces[d], "row", 2 * d) for d in range(1, chips)]

    def gather(piece):
        same = [piece] + [swap(piece, "row", 2 * d) for d in range(1, chips)]
        chunks = same + [swap(part, "row", 1) for part in same]
        return chunks if aligned else [jnp.concatenate(chunks, axis=0)]

    coeffs = pl.pallas_call(
        functools.partial(columns_kernel, chans),
        name="columns",
        grid=(blocks,),
        in_specs=[block, whole((width, lanes))],
        out_specs=pl.BlockSpec((GROUP, flat), lambda i: (i, 0)),
        out_shape=jax.ShapeDtypeStruct((rows_here, flat), BF16),
    )(field, forward)
    chunks = spread(rows_step(coeffs, swap(coeffs, "row", 1), False))

    mixed, spectrum = pl.pallas_call(
        functools.partial(mix_kernel, chans, modes, chips),
        name="mix",
        out_shape=[jax.ShapeDtypeStruct((owned, flat), BF16)] * 2,
        scratch_shapes=[pltpu.VMEM((2 * chans, owned, modes), F32)],
    )(spectral, *chunks)
    mixed = gather(mixed)
    spectra = [spectrum] + [swap(spectrum, "dp", d) for d in range(1, map_count)]

    tile = min(512, width)
    chunk_specs = [whole(part.shape) for part in mixed]
    grad_pre, grad_coeffs = pl.pallas_call(
        functools.partial(main_kernel, chans, modes, scale, tile, len(mixed)),
        name="main",
        grid=(blocks,),
        in_specs=chunk_specs
        + [
            whole(to_rows.shape),
            whole(inverse.shape),
            whole(forward.shape),
            whole((chans, chans)),
            whole((1, chans)),
            block,
            block,
        ],
        out_specs=[block, whole((rows_here, flat + LANES))],
        out_shape=[
            jax.ShapeDtypeStruct(field.shape, BF16),
            jax.ShapeDtypeStruct((rows_here, flat + LANES), BF16),
        ],
        scratch_shapes=[
            pltpu.VMEM((blocks, size, lanes), BF16),
            pltpu.VMEM((size, size), BF16),
            pltpu.VMEM((size, size), F32),
            pltpu.VMEM((size, modes), F32),
        ],
    )(*mixed, to_rows, inverse, forward, local_weight, bias[None], field, cot)

    chunks = spread(rows_step(grad_coeffs, swap(grad_coeffs, "row", 1), True))
    part_lanes = chans // map_count * lanes
    outs = pl.pallas_call(
        functools.partial(back_kernel, chans, modes, chips, map_count),
        name="back",
        in_specs=[pl.BlockSpec(memory_space=pltpu.SMEM)]
        + [pl.BlockSpec(memory_space=pltpu.VMEM)] * (1 + chips),
        out_shape=[jax.ShapeDtypeStruct((owned, flat), BF16)]
        + [jax.ShapeDtypeStruct((owned, part_lanes + extra), BF16)] * map_count,
        scratch_shapes=[
            pltpu.VMEM((2 * chans, owned, modes), F32),
            pltpu.VMEM((owned, flat), BF16),
        ],
    )(lax.axis_index("dp").astype(jnp.int32)[None], spectral, *chunks)
    freq_grad = gather(outs[0])
    slices = [outs[1]] + [swap(outs[1 + d], "dp", d) for d in range(1, map_count)]

    spectral_grad, small = pl.pallas_call(
        functools.partial(weight_kernel, chans, modes, map_count, grad_scale),
        name="weights",
        out_shape=[
            jax.ShapeDtypeStruct((2, chans, chans // map_count, owned, modes), F32),
            jax.ShapeDtypeStruct((chans, LANES), F32),
        ],
    )(*spectra, *slices)

    field_grad = pl.pallas_call(
        functools.partial(field_kernel, chans, modes, scale, tile, len(freq_grad)),
        name="field",
        grid=(blocks,),
        in_specs=[whole(part.shape) for part in freq_grad]
        + [whole(to_rows.shape), whole(inverse.shape), whole((chans, chans)), block],
        out_specs=block,
        out_shape=jax.ShapeDtypeStruct(field.shape, BF16),
        scratch_shapes=[
            pltpu.VMEM((blocks, size, lanes), BF16),
            pltpu.VMEM((size, size), BF16),
        ],
    )(*freq_grad, to_rows, inverse, local_weight, grad_pre)

    return (field_grad[None], spectral_grad, small[:, :chans], small[:, chans])


def solution(mesh):
    return jax.shard_map(
        on_device,
        mesh=mesh,
        in_specs=(
            P("dp", None, "row", None),
            P("dp", None, "row", None),
            P(None, None, None, "row", None),
            P(),
            P(),
        ),
        out_specs=(P("dp", None, "row", None), P(None, None, "dp", "row", None), P(), P()),
        check_vma=False,
    )
```

```python
import functools
import math

import jax
import jax.numpy as jnp
import numpy as np
from jax import lax
from jax.experimental import pallas as pl
from jax.experimental.pallas import tpu as pltpu
from jax.sharding import PartitionSpec as P


BF16 = jnp.bfloat16
F32 = jnp.float32
LANES = 128
TILE = 512
GROUP = 16


def column_table(width, modes):
    turns = np.arange(modes)[:, None] * np.arange(width)[None, :] % width
    angle = np.float32(2.0 * math.pi / width) * turns.astype(np.float32)
    table = np.concatenate([np.cos(angle), -np.sin(angle)], axis=0)
    return table.astype(BF16)


def row_angles(mode, place, height, modes):
    freq = (mode - modes // 2) % height
    turns = freq[:, None] * place[None, :] % height
    return 2.0 * math.pi / height * turns.astype(F32)


def dot(left, right):
    return jnp.dot(left, right, preferred_element_type=F32)


def dot_nt(left, right):
    return lax.dot_general(left, right, (((1,), (1,)), ((), ())), preferred_element_type=F32)


def tree(parts):
    parts = list(parts)
    while len(parts) > 1:
        parts = [parts[at] + parts[at + 1] for at in range(0, len(parts), 2)]
    return parts[0]


def whole(shape):
    return pl.BlockSpec(shape, lambda *_: (0,) * len(shape))


def room(mebibytes):
    return pltpu.CompilerParams(vmem_limit_bytes=mebibytes << 20)


def streamed(value):
    return pltpu.with_memory_space_constraint(value, pltpu.HBM)


def to_pieces(value):
    first = value.astype(BF16).astype(F32)
    rest = value - first
    second = rest.astype(BF16).astype(F32)
    third = rest - second
    return first + pltpu.roll(second, 32, 1) + pltpu.roll(third, 64, 1)


def from_pieces(packed):
    back = LANES
    return packed + pltpu.roll(packed, back - 32, 1) + pltpu.roll(packed, back - 64, 1)


def columns_kernel(field_ref, table_ref, out_ref, total):
    chans, rows, tile = field_ref.shape
    lanes = table_ref.shape[1]
    step = pl.program_id(0)
    part = dot(field_ref[...].reshape(chans * rows, tile), table_ref[...])

    @pl.when(step == 0)
    def _():
        total[...] = part

    @pl.when(step > 0)
    def _():
        total[...] += part

    @pl.when(step == pl.num_programs(0) - 1)
    def _():
        for c in range(chans):
            out_ref[:, c * lanes : (c + 1) * lanes] = total[c * rows : (c + 1) * rows].astype(BF16)


def rows_kernel(chans, modes, scale, extra, mine_ref, other_ref, phase_ref, *outs):
    half = phase_ref.shape[0] // 2
    lanes = 2 * modes
    phase = phase_ref[...]
    for c in range(chans):
        at = slice(c * lanes, (c + 1) * lanes)
        both = jnp.concatenate([mine_ref[:, at], other_ref[:, at]], axis=0)
        part = dot(phase, both)
        real = part[:half, :modes] + part[half:, modes:]
        imag = part[:half, modes:] - part[half:, :modes]
        full = (scale * jnp.concatenate([real, imag], axis=1)).astype(BF16)
        size = half // len(outs)
        for d, out in enumerate(outs):
            out[:, at] = full[d * size : (d + 1) * size]
    if extra:
        top = chans * lanes
        rows = chans
        total = from_pieces(mine_ref[:rows, top:].astype(F32)) + from_pieces(
            other_ref[:rows, top:].astype(F32)
        )
        packed = to_pieces(keep_low(total)).astype(BF16)
        for out in outs:
            put_pieces(out, packed, top, rows)


def keep_low(value):
    lane = lax.broadcasted_iota(jnp.int32, value.shape, 1)
    return jnp.where(lane < 32, value, 0.0)


def put_pieces(out, packed, top, rows):
    size = out.shape[0]
    if size >= rows:
        out[:rows, top : top + LANES] = packed
        if size > rows:
            out[rows:, top : top + LANES] = jnp.zeros((size - rows, LANES), packed.dtype)
        return
    for e in range(rows // size):
        out[:, top + e * LANES : top + (e + 1) * LANES] = packed[e * size : (e + 1) * size]


def get_pieces(ref, top, rows):
    size = ref.shape[0]
    if size >= rows:
        return ref[:rows, top : top + LANES].astype(F32)
    return jnp.concatenate(
        [
            ref[:, top + e * LANES : top + (e + 1) * LANES].astype(F32)
            for e in range(rows // size)
        ],
        axis=0,
    )


def mix_kernel(chans, modes, count, weight_ref, *refs):
    chunks = refs[:count]
    mixed_ref, spectrum_ref, sums = refs[count:]
    lanes = 2 * modes
    for c in range(2 * chans):
        at = slice(c * modes, (c + 1) * modes)
        value = tree([chunk[:, at].astype(F32) for chunk in chunks])
        sums[c] = value
        spectrum_ref[:, at] = value.astype(BF16)

    for o in range(chans):
        real = imag = None
        for c in range(chans):
            wr = weight_ref[0, c, o].astype(F32)
            wi = weight_ref[1, c, o].astype(F32)
            fr = sums[2 * c]
            fi = sums[2 * c + 1]
            a = wr * fr - wi * fi
            b = wr * fi + wi * fr
            real = a if real is None else real + a
            imag = b if imag is None else imag + b
        mixed_ref[:, o * lanes : o * lanes + modes] = real.astype(BF16)
        mixed_ref[:, o * lanes + modes : (o + 1) * lanes] = imag.astype(BF16)


def back_kernel(chans, modes, count, maps, where_ref, weight_ref, *refs):
    chunks = refs[:count]
    back_ref = refs[count]
    slices = refs[count + 1 : count + 1 + maps]
    sums, gathered = refs[count + 1 + maps :]
    lanes = 2 * modes
    shape = (chunks[0].shape[0], modes)
    doubling = jnp.where(lax.broadcasted_iota(jnp.int32, shape, 1) == 0, 1.0, 2.0)
    for c in range(2 * chans):
        at = slice(c * modes, (c + 1) * modes)
        value = tree([chunk[:, at].astype(F32) for chunk in chunks]) * doubling
        sums[c] = value
        gathered[:, at] = value.astype(BF16)

    for c in range(chans):
        real = imag = None
        for o in range(chans):
            wr = weight_ref[0, c, o].astype(F32)
            wi = weight_ref[1, c, o].astype(F32)
            gr = sums[2 * o]
            gi = sums[2 * o + 1]
            a = wr * gr + wi * gi
            b = wr * gi - wi * gr
            real = a if real is None else real + a
            imag = b if imag is None else imag + b
        back_ref[:, c * lanes : c * lanes + modes] = real.astype(BF16)
        back_ref[:, c * lanes + modes : (c + 1) * lanes] = imag.astype(BF16)

    top = chans * lanes
    total = tree([from_pieces(get_pieces(chunk, top, chans)) for chunk in chunks])
    packed = to_pieces(keep_low(total)).astype(BF16)
    span = chans // maps * lanes
    for d, out in enumerate(slices):
        first = pl.multiple_of((where_ref[0] ^ d) * span, LANES)
        out[:, :span] = gathered[:, pl.ds(first, span)]
        put_pieces(out, packed, span, chans)


def weight_kernel(chans, modes, maps, scale, *refs):
    spectra = refs[:maps]
    slices = refs[maps : 2 * maps]
    grad_ref, local_ref, bias_ref = refs[2 * maps :]
    lanes = 2 * modes
    part = chans // maps
    for o in range(part):
        at = o * lanes
        grads = [
            (s[:, at : at + modes].astype(F32), s[:, at + modes : at + lanes].astype(F32))
            for s in slices
        ]
        for c in range(grad_ref.shape[1]):
            at = c * lanes
            real = []
            imag = []
            for spectrum, (gr, gi) in zip(spectra, grads):
                fr = spectrum[:, at : at + modes].astype(F32)
                fi = spectrum[:, at + modes : at + lanes].astype(F32)
                real.append(gr * fr + gi * fi)
                imag.append(gi * fr - gr * fi)
            grad_ref[0, c, o] = tree(real)
            grad_ref[1, c, o] = tree(imag)

    @pl.when(pl.program_id(0) == 0)
    def _():
        small = [from_pieces(get_pieces(s, part * lanes, chans)) for s in slices]
        small = scale * tree(small)
        local_ref[...] = small[:, :chans]
        bias_ref[...] = pltpu.roll(small, LANES - chans, 1)[:1, :chans]


def channel_map(local_ref, chans, back):
    size = chans * GROUP
    pick = (
        lax.broadcasted_iota(jnp.int32, (size, chans), 0) // GROUP
        == lax.broadcasted_iota(jnp.int32, (size, chans), 1)
    )
    pick = jnp.where(pick, 1.0, 0.0).astype(BF16)
    local = local_ref[...]
    if back:
        wide = dot(pick, local).astype(BF16)
    else:
        wide = lax.dot_general(
            pick, local, (((1,), (1,)), ((), ())), preferred_element_type=F32
        ).astype(BF16)
    full = dot_nt(wide, pick)
    row = lax.broadcasted_iota(jnp.int32, (size, size), 0) % GROUP
    lane = lax.broadcasted_iota(jnp.int32, (size, size), 1) % GROUP
    return jnp.where(row == lane, full, 0.0).astype(BF16)


def inverse_rows(chans, modes, scale, phase, chunks, doubled, out):
    lanes = 2 * modes
    half = phase.shape[0] // 2
    factor = jnp.full((1, modes), scale, F32)
    if doubled:
        first = lax.broadcasted_iota(jnp.int32, (1, modes), 1) == 0
        factor = jnp.where(first, scale, 2.0 * scale)
    for o in range(chans):
        at = slice(o * lanes, (o + 1) * lanes)
        part = dot(phase, jnp.concatenate([chunk[:, at] for chunk in chunks], axis=0))
        real = (part[:half, :modes] - part[half:, modes:]) * factor
        imag = (part[:half, modes:] + part[half:, :modes]) * factor
        out[o * half : (o + 1) * half, :modes] = real.astype(BF16)
        out[o * half : (o + 1) * half, modes:] = imag.astype(BF16)


SLOPE = math.sqrt(2.0 / math.pi)
CUBIC = 0.044715


def gelu_slope(x):
    kind = x.dtype.type
    square = x * x
    inner = x * (kind(SLOPE) + kind(SLOPE * CUBIC) * square)
    outer = x * (kind(0.5 * SLOPE) + kind(1.5 * SLOPE * CUBIC) * square)
    t = jnp.tanh(inner)
    return (kind(1.0) + t) * (kind(0.5) + (kind(1.0) - t) * outer)


def main_kernel(chans, modes, scale, count, *refs):
    chunks = refs[:count]
    (phase_ref, inverse_ref, forward_ref, local_ref, bias_ref, field_ref, cot_ref) = refs[
        count : count + 7
    ]
    grad_ref, sums_ref, rows, mixer, wide, total, outer = refs[count + 7 :]
    step = pl.program_id(0)
    size = chans * GROUP
    here, tile = field_ref.shape[1:]
    lanes = 2 * modes

    @pl.when(step == 0)
    def _():
        inverse_rows(chans, modes, scale, phase_ref[...], chunks, True, rows)
        mixer[...] = channel_map(local_ref, chans, False)
        total[...] = jnp.zeros_like(total)
        outer[...] = jnp.zeros_like(outer)
        sums_ref[...] = jnp.zeros_like(sums_ref)

    mix = mixer[...]
    group = lax.broadcasted_iota(jnp.int32, (size, chans), 0) // GROUP
    pick = group == lax.broadcasted_iota(jnp.int32, (size, chans), 1)
    bias = jnp.sum(jnp.where(pick, bias_ref[...], 0.0), axis=1, keepdims=True)
    wide[...] = dot(rows[...], inverse_ref[...]).reshape(chans, here, tile)
    both = jnp.zeros((size, size), F32)
    for at in range(0, here, GROUP):
        block = slice(at, at + GROUP)
        field = field_ref[:, block, :].reshape(size, tile)
        preact = dot(mix, field) + wide[:, block, :].reshape(size, tile) + bias
        cot = cot_ref[:, block, :].reshape(size, tile)
        grad = cot * gelu_slope(preact.astype(BF16))
        grad_ref[:, block, :] = grad.reshape(chans, GROUP, tile)
        both = both + dot_nt(field, grad)
    outer[...] += both
    total[...] += dot(grad_ref[...].reshape(chans * here, tile), forward_ref[...])

    @pl.when(step == pl.num_programs(0) - 1)
    def _():
        for o in range(chans):
            sums_ref[:, o * lanes : (o + 1) * lanes] = total[o * here : (o + 1) * here].astype(BF16)
        row = lax.broadcasted_iota(jnp.int32, (size, size), 0) % GROUP
        lane = lax.broadcasted_iota(jnp.int32, (size, size), 1) % GROUP
        same = jnp.where(row == lane, outer[...], 0.0).reshape(chans, GROUP, size)
        folded = jnp.sum(same, axis=1)
        wider = lax.broadcasted_iota(jnp.int32, (size, LANES), 0) // GROUP
        gather = wider == lax.broadcasted_iota(jnp.int32, (size, LANES), 1)
        local = jnp.dot(
            folded,
            jnp.where(gather, 1.0, 0.0),
            precision=lax.Precision.HIGHEST,
            preferred_element_type=F32,
        )
        biases = jnp.sum(total[:, :modes].reshape(chans, here, modes), axis=1)[:, :1]
        place = lax.broadcasted_iota(jnp.int32, (chans, LANES), 1)
        line = lax.broadcasted_iota(jnp.int32, (chans, LANES), 0)
        across = jnp.sum(jnp.where(place == chans + line, biases, 0.0), axis=0, keepdims=True)
        small = jnp.where(place < chans, local, jnp.where(line == 0, across, 0.0))
        sums_ref[:chans, chans * lanes :] = to_pieces(small).astype(BF16)


def field_kernel(chans, modes, scale, count, *refs):
    chunks = refs[:count]
    phase_ref, inverse_ref, local_ref, grad_ref, out_ref, rows, mixer, wide = refs[count:]
    size = chans * GROUP
    here, tile = grad_ref.shape[1:]

    @pl.when(pl.program_id(0) == 0)
    def _():
        inverse_rows(chans, modes, scale, phase_ref[...], chunks, False, rows)
        mixer[...] = channel_map(local_ref, chans, True)

    mix = mixer[...]
    wide[...] = dot(rows[...], inverse_ref[...]).reshape(chans, here, tile)
    for at in range(0, here, GROUP):
        block = slice(at, at + GROUP)
        value = dot(mix, grad_ref[:, block, :].reshape(size, tile))
        value = value + wide[:, block, :].reshape(size, tile)
        out_ref[:, block, :] = value.astype(BF16).reshape(chans, GROUP, tile)


def swap(value, axis, mask):
    size = lax.axis_size(axis)
    return lax.ppermute(value, axis, [(at, at ^ mask) for at in range(size)])


def on_device(fields, cotangent, spectral, local_weight, bias):
    field = fields[0]
    cot = cotangent[0]
    chans, rows_here, width = field.shape
    owned, modes = spectral.shape[3:]
    row_count = lax.axis_size("row")
    map_count = lax.axis_size("dp")
    chips = row_count // 2
    height = rows_here * row_count
    scale = 1.0 / math.sqrt(height * width)
    grad_scale = 1.0 / math.sqrt(map_count * height * width)
    lanes = 2 * modes
    flat = chans * lanes
    size = chans * GROUP
    extra = LANES * max(1, chans // owned)
    assert 2 * chans <= 32
    aligned = owned % GROUP == 0

    me = lax.axis_index("row")
    chip, core = me // 2, me % 2
    inverse_const = column_table(width, modes)
    inverse = jnp.asarray(inverse_const)
    forward = jnp.asarray(np.ascontiguousarray(inverse_const.T))

    near = jnp.arange(chips, dtype=jnp.int32) ^ chip
    inner = jnp.arange(owned, dtype=jnp.int32)
    own_modes = ((2 * near + core)[:, None] * owned + inner[None, :]).reshape(-1)
    far_modes = ((2 * near + 1 - core)[:, None] * owned + inner[None, :]).reshape(-1)
    here = jnp.arange(rows_here, dtype=jnp.int32)
    pair_rows = jnp.concatenate([me * rows_here + here, (me ^ 1) * rows_here + here])
    angle = row_angles(own_modes, pair_rows, height, modes)
    to_modes = jnp.concatenate([jnp.cos(angle), jnp.sin(angle)], axis=0).astype(BF16)
    all_modes = jnp.concatenate([own_modes, far_modes])
    angle = row_angles(all_modes, me * rows_here + here, height, modes).T
    to_rows = jnp.concatenate([jnp.cos(angle), jnp.sin(angle)], axis=0).astype(BF16)

    tile = min(TILE, width)
    tiles = width // tile
    block = pl.BlockSpec((chans, rows_here, tile), lambda i: (0, 0, i))
    inverse_block = pl.BlockSpec((lanes, tile), lambda i: (0, i))
    forward_block = pl.BlockSpec((tile, lanes), lambda i: (i, 0))

    def rows_step(mine, other, more):
        out_lanes = flat + (extra if more else 0)
        if aligned:
            shapes = [jax.ShapeDtypeStruct((owned, out_lanes), BF16)] * chips
        else:
            shapes = [jax.ShapeDtypeStruct((chips * owned, flat), BF16)]
        kernel = functools.partial(rows_kernel, chans, modes, scale, more and aligned)
        outs = pl.pallas_call(
            kernel,
            name="rows",
            out_shape=shapes,
            compiler_params=room(8),
            cost_estimate=pl.CostEstimate(
                flops=4 * chips * owned * 2 * rows_here * flat,
                transcendentals=0,
                bytes_accessed=6 * rows_here * flat,
            ),
        )(mine, other, to_modes)
        if aligned:
            return outs
        pieces = jnp.split(outs[0], chips, axis=0)
        if more:
            packed = small_sum(mine[:chans, flat:], other[:chans, flat:])
            packed = packed.reshape(chans // owned, owned, LANES).transpose(1, 0, 2)
            packed = packed.reshape(owned, extra)
            pieces = [jnp.concatenate([piece, packed], axis=1) for piece in pieces]
        return pieces

    def small_sum(mine, other):
        def kernel(a, b, out):
            total = from_pieces(a[...].astype(F32)) + from_pieces(b[...].astype(F32))
            out[...] = to_pieces(keep_low(total)).astype(BF16)

        return pl.pallas_call(
            kernel, name="small", out_shape=jax.ShapeDtypeStruct((chans, LANES), BF16)
        )(mine, other)

    def spread(pieces):
        return [pieces[0]] + [swap(pieces[d], "row", 2 * d) for d in range(1, chips)]

    def gather(piece):
        same = [piece] + [swap(piece, "row", 2 * d) for d in range(1, chips)]
        chunks = same + [swap(part, "row", 1) for part in same]
        return chunks if aligned else [jnp.concatenate(chunks, axis=0)]

    coeffs = pl.pallas_call(
        columns_kernel,
        name="columns",
        grid=(tiles,),
        in_specs=[block, forward_block],
        out_specs=whole((rows_here, flat)),
        out_shape=jax.ShapeDtypeStruct((rows_here, flat), BF16),
        scratch_shapes=[pltpu.VMEM((chans * rows_here, lanes), F32)],
        compiler_params=room(12),
    )(streamed(field), streamed(forward))
    chunks = spread(rows_step(coeffs, swap(coeffs, "row", 1), False))

    mixed, spectrum = pl.pallas_call(
        functools.partial(mix_kernel, chans, modes, chips),
        name="mix",
        out_shape=[jax.ShapeDtypeStruct((owned, flat), BF16)] * 2,
        scratch_shapes=[pltpu.VMEM((2 * chans, owned, modes), F32)],
        compiler_params=room(10),
    )(spectral, *chunks)
    mixed = gather(mixed)
    spectra = [spectrum] + [swap(spectrum, "dp", d) for d in range(1, map_count)]

    chunk_specs = [whole(part.shape) for part in mixed]
    main = pl.pallas_call(
        functools.partial(main_kernel, chans, modes, scale, len(mixed)),
        name="main",
        grid=(tiles,),
        in_specs=chunk_specs
        + [
            whole(to_rows.shape),
            inverse_block,
            forward_block,
            whole((chans, chans)),
            whole((1, chans)),
            block,
            block,
        ],
        out_specs=[block, whole((rows_here, flat + LANES))],
        out_shape=[
            pltpu.HBM(field.shape, BF16),
            jax.ShapeDtypeStruct((rows_here, flat + LANES), BF16),
        ],
        scratch_shapes=[
            pltpu.VMEM((chans * rows_here, lanes), BF16),
            pltpu.VMEM((size, size), BF16),
            pltpu.VMEM((chans, rows_here, tile), F32),
            pltpu.VMEM((chans * rows_here, lanes), F32),
            pltpu.VMEM((size, size), F32),
        ],
        compiler_params=room(28),
    )
    grad_pre, grad_coeffs = main(
        *mixed, to_rows, streamed(inverse), streamed(forward), local_weight, bias[None], streamed(field), streamed(cot)
    )

    chunks = spread(rows_step(grad_coeffs, swap(grad_coeffs, "row", 1), True))
    part_lanes = chans // map_count * lanes
    outs = pl.pallas_call(
        functools.partial(back_kernel, chans, modes, chips, map_count),
        name="back",
        in_specs=[pl.BlockSpec(memory_space=pltpu.SMEM)]
        + [pl.BlockSpec(memory_space=pltpu.VMEM)] * (1 + chips),
        out_shape=[jax.ShapeDtypeStruct((owned, flat), BF16)]
        + [jax.ShapeDtypeStruct((owned, part_lanes + extra), BF16)] * map_count,
        scratch_shapes=[
            pltpu.VMEM((2 * chans, owned, modes), F32),
            pltpu.VMEM((owned, flat), BF16),
        ],
        compiler_params=room(10),
    )(lax.axis_index("dp").astype(jnp.int32)[None], spectral, *chunks)
    freq_grad = gather(outs[0])
    slices = [outs[1]] + [swap(outs[1 + d], "dp", d) for d in range(1, map_count)]

    steps = 4 if chans % 4 == 0 else 1
    spectral_grad, local_grad, bias_grad = pl.pallas_call(
        functools.partial(weight_kernel, chans, modes, map_count, grad_scale),
        name="weights",
        grid=(steps,),
        in_specs=[pl.BlockSpec((owned, flat // steps), lambda i: (0, i))] * map_count
        + [whole(slices[0].shape)] * map_count,
        out_specs=[
            pl.BlockSpec(
                (2, chans // steps, chans // map_count, owned, modes), lambda i: (0, i, 0, 0, 0)
            ),
            whole((chans, chans)),
            whole((1, chans)),
        ],
        out_shape=[
            pltpu.HBM((2, chans, chans // map_count, owned, modes), F32),
            jax.ShapeDtypeStruct((chans, chans), F32),
            jax.ShapeDtypeStruct((1, chans), F32),
        ],
        compiler_params=room(12),
    )(*spectra, *slices)

    final = pl.pallas_call(
        functools.partial(field_kernel, chans, modes, scale, len(freq_grad)),
        name="field",
        grid=(tiles,),
        in_specs=[whole(part.shape) for part in freq_grad]
        + [whole(to_rows.shape), inverse_block, whole((chans, chans)), block],
        out_specs=block,
        out_shape=pltpu.HBM(field.shape, BF16),
        scratch_shapes=[
            pltpu.VMEM((chans * rows_here, lanes), BF16),
            pltpu.VMEM((size, size), BF16),
            pltpu.VMEM((chans, rows_here, tile), F32),
        ],
        compiler_params=room(20),
    )
    field_grad = final(
        *freq_grad, to_rows, streamed(inverse), local_weight, streamed(grad_pre)
    )

    return (field_grad[None], spectral_grad, local_grad, bias_grad[0])


def solution(mesh):
    return jax.shard_map(
        on_device,
        mesh=mesh,
        in_specs=(
            P("dp", None, "row", None),
            P("dp", None, "row", None),
            P(None, None, None, "row", None),
            P(),
            P(),
        ),
        out_specs=(P("dp", None, "row", None), P(None, None, "dp", "row", None), P(), P()),
        check_vma=False,
    )
```

```python
import functools
import math

import jax
import jax.numpy as jnp
import numpy as np
from jax import lax
from jax.experimental import pallas as pl
from jax.experimental.pallas import tpu as pltpu
from jax.sharding import PartitionSpec as P


BF16 = jnp.bfloat16
F32 = jnp.float32
LANES = 128
TILE = 1024
MAIN_TILE = 512
GROUP = 16


def column_table(width, modes):
    turns = np.arange(modes)[:, None] * np.arange(width)[None, :] % width
    angle = np.float32(2.0 * math.pi / width) * turns.astype(np.float32)
    table = np.concatenate([np.cos(angle), -np.sin(angle)], axis=0)
    return table.astype(BF16)


def row_angles(mode, place, height, modes):
    freq = (mode - modes // 2) % height
    turns = freq[:, None] * place[None, :] % height
    return 2.0 * math.pi / height * turns.astype(F32)


def dot(left, right):
    return jnp.dot(left, right, preferred_element_type=F32)


def dot_nt(left, right):
    return lax.dot_general(left, right, (((1,), (1,)), ((), ())), preferred_element_type=F32)


def tree(parts):
    parts = list(parts)
    while len(parts) > 1:
        parts = [parts[at] + parts[at + 1] for at in range(0, len(parts), 2)]
    return parts[0]


def whole(shape):
    return pl.BlockSpec(shape, lambda *_: (0,) * len(shape))


def room(mebibytes):
    return pltpu.CompilerParams(vmem_limit_bytes=mebibytes << 20)


def streamed(value):
    return pltpu.with_memory_space_constraint(value, pltpu.HBM)


def to_pieces(value):
    first = value.astype(BF16).astype(F32)
    rest = value - first
    second = rest.astype(BF16).astype(F32)
    third = rest - second
    return first + pltpu.roll(second, 32, 1) + pltpu.roll(third, 64, 1)


def from_pieces(packed):
    back = LANES
    return packed + pltpu.roll(packed, back - 32, 1) + pltpu.roll(packed, back - 64, 1)


def columns_kernel(field_ref, table_ref, out_ref, total):
    chans, rows, tile = field_ref.shape
    lanes = table_ref.shape[1]
    step = pl.program_id(0)
    part = dot(field_ref[...].reshape(chans * rows, tile), table_ref[...])

    @pl.when(step == 0)
    def _():
        total[...] = part

    @pl.when(step > 0)
    def _():
        total[...] += part

    @pl.when(step == pl.num_programs(0) - 1)
    def _():
        for c in range(chans):
            out_ref[:, c * lanes : (c + 1) * lanes] = total[c * rows : (c + 1) * rows].astype(BF16)


def rows_kernel(chans, modes, scale, extra, mine_ref, other_ref, phase_ref, *outs):
    half = phase_ref.shape[0] // 2
    lanes = 2 * modes
    phase = phase_ref[...]
    for c in range(chans):
        at = slice(c * lanes, (c + 1) * lanes)
        both = jnp.concatenate([mine_ref[:, at], other_ref[:, at]], axis=0)
        part = dot(phase, both)
        real = part[:half, :modes] + part[half:, modes:]
        imag = part[:half, modes:] - part[half:, :modes]
        full = (scale * jnp.concatenate([real, imag], axis=1)).astype(BF16)
        size = half // len(outs)
        for d, out in enumerate(outs):
            out[:, at] = full[d * size : (d + 1) * size]
    if extra:
        top = chans * lanes
        rows = chans
        total = from_pieces(mine_ref[:rows, top:].astype(F32)) + from_pieces(
            other_ref[:rows, top:].astype(F32)
        )
        packed = to_pieces(keep_low(total)).astype(BF16)
        for out in outs:
            put_pieces(out, packed, top, rows)


def keep_low(value):
    lane = lax.broadcasted_iota(jnp.int32, value.shape, 1)
    return jnp.where(lane < 32, value, 0.0)


def put_pieces(out, packed, top, rows):
    size = out.shape[0]
    if size >= rows:
        out[:rows, top : top + LANES] = packed
        if size > rows:
            out[rows:, top : top + LANES] = jnp.zeros((size - rows, LANES), packed.dtype)
        return
    for e in range(rows // size):
        out[:, top + e * LANES : top + (e + 1) * LANES] = packed[e * size : (e + 1) * size]


def get_pieces(ref, top, rows):
    size = ref.shape[0]
    if size >= rows:
        return ref[:rows, top : top + LANES].astype(F32)
    return jnp.concatenate(
        [
            ref[:, top + e * LANES : top + (e + 1) * LANES].astype(F32)
            for e in range(rows // size)
        ],
        axis=0,
    )


def mix_kernel(chans, modes, count, weight_ref, *refs):
    chunks = refs[:count]
    mixed_ref, spectrum_ref, sums = refs[count:]
    lanes = 2 * modes
    for c in range(2 * chans):
        at = slice(c * modes, (c + 1) * modes)
        value = tree([chunk[:, at].astype(F32) for chunk in chunks])
        sums[c] = value
        spectrum_ref[:, at] = value.astype(BF16)

    for o in range(chans):
        real = imag = None
        for c in range(chans):
            wr = weight_ref[0, c, o].astype(F32)
            wi = weight_ref[1, c, o].astype(F32)
            fr = sums[2 * c]
            fi = sums[2 * c + 1]
            a = wr * fr - wi * fi
            b = wr * fi + wi * fr
            real = a if real is None else real + a
            imag = b if imag is None else imag + b
        mixed_ref[:, o * lanes : o * lanes + modes] = real.astype(BF16)
        mixed_ref[:, o * lanes + modes : (o + 1) * lanes] = imag.astype(BF16)


def back_kernel(chans, modes, count, maps, where_ref, weight_ref, *refs):
    chunks = refs[:count]
    back_ref = refs[count]
    slices = refs[count + 1 : count + 1 + maps]
    sums, gathered = refs[count + 1 + maps :]
    lanes = 2 * modes
    shape = (chunks[0].shape[0], modes)
    doubling = jnp.where(lax.broadcasted_iota(jnp.int32, shape, 1) == 0, 1.0, 2.0)
    for c in range(2 * chans):
        at = slice(c * modes, (c + 1) * modes)
        value = tree([chunk[:, at].astype(F32) for chunk in chunks]) * doubling
        sums[c] = value
        gathered[:, at] = value.astype(BF16)

    for c in range(chans):
        real = imag = None
        for o in range(chans):
            wr = weight_ref[0, c, o].astype(F32)
            wi = weight_ref[1, c, o].astype(F32)
            gr = sums[2 * o]
            gi = sums[2 * o + 1]
            a = wr * gr + wi * gi
            b = wr * gi - wi * gr
            real = a if real is None else real + a
            imag = b if imag is None else imag + b
        back_ref[:, c * lanes : c * lanes + modes] = real.astype(BF16)
        back_ref[:, c * lanes + modes : (c + 1) * lanes] = imag.astype(BF16)

    top = chans * lanes
    total = tree([from_pieces(get_pieces(chunk, top, chans)) for chunk in chunks])
    packed = to_pieces(keep_low(total)).astype(BF16)
    span = chans // maps * lanes
    for d, out in enumerate(slices):
        first = pl.multiple_of((where_ref[0] ^ d) * span, LANES)
        out[:, :span] = gathered[:, pl.ds(first, span)]
        put_pieces(out, packed, span, chans)


def weight_kernel(chans, modes, maps, scale, *refs):
    spectra = refs[:maps]
    slices = refs[maps : 2 * maps]
    grad_ref, local_ref, bias_ref = refs[2 * maps :]
    lanes = 2 * modes
    part = chans // maps
    for o in range(part):
        at = o * lanes
        grads = [
            (s[:, at : at + modes].astype(F32), s[:, at + modes : at + lanes].astype(F32))
            for s in slices
        ]
        for c in range(grad_ref.shape[1]):
            at = c * lanes
            real = []
            imag = []
            for spectrum, (gr, gi) in zip(spectra, grads):
                fr = spectrum[:, at : at + modes].astype(F32)
                fi = spectrum[:, at + modes : at + lanes].astype(F32)
                real.append(gr * fr + gi * fi)
                imag.append(gi * fr - gr * fi)
            grad_ref[0, c, o] = tree(real)
            grad_ref[1, c, o] = tree(imag)

    @pl.when(pl.program_id(0) == 0)
    def _():
        small = [from_pieces(get_pieces(s, part * lanes, chans)) for s in slices]
        small = scale * tree(small)
        local_ref[...] = small[:, :chans]
        bias_ref[...] = pltpu.roll(small, LANES - chans, 1)[:1, :chans]


def channel_map(local_ref, chans, back):
    size = chans * GROUP
    pick = (
        lax.broadcasted_iota(jnp.int32, (size, chans), 0) // GROUP
        == lax.broadcasted_iota(jnp.int32, (size, chans), 1)
    )
    pick = jnp.where(pick, 1.0, 0.0).astype(BF16)
    local = local_ref[...]
    if back:
        wide = dot(pick, local).astype(BF16)
    else:
        wide = lax.dot_general(
            pick, local, (((1,), (1,)), ((), ())), preferred_element_type=F32
        ).astype(BF16)
    full = dot_nt(wide, pick)
    row = lax.broadcasted_iota(jnp.int32, (size, size), 0) % GROUP
    lane = lax.broadcasted_iota(jnp.int32, (size, size), 1) % GROUP
    return jnp.where(row == lane, full, 0.0).astype(BF16)


def inverse_rows(chans, modes, scale, phase, chunks, doubled, out):
    lanes = 2 * modes
    half = phase.shape[0] // 2
    factor = jnp.full((1, modes), scale, F32)
    if doubled:
        first = lax.broadcasted_iota(jnp.int32, (1, modes), 1) == 0
        factor = jnp.where(first, scale, 2.0 * scale)
    for o in range(chans):
        at = slice(o * lanes, (o + 1) * lanes)
        part = dot(phase, jnp.concatenate([chunk[:, at] for chunk in chunks], axis=0))
        real = ((part[:half, :modes] - part[half:, modes:]) * factor).astype(BF16)
        imag = ((part[:half, modes:] + part[half:, :modes]) * factor).astype(BF16)
        for at in range(0, half, GROUP):
            first = at * chans + o * GROUP
            out[first : first + GROUP, :modes] = real[at : at + GROUP]
            out[first : first + GROUP, modes:] = imag[at : at + GROUP]


SLOPE = math.sqrt(2.0 / math.pi)
CUBIC = 0.044715


def gelu_slope(x):
    kind = x.dtype.type
    square = x * x
    inner = x * (kind(SLOPE) + kind(SLOPE * CUBIC) * square)
    outer = x * (kind(0.5 * SLOPE) + kind(1.5 * SLOPE * CUBIC) * square)
    t = jnp.tanh(inner)
    return (kind(1.0) + t) * (kind(0.5) + (kind(1.0) - t) * outer)


def main_kernel(chans, modes, scale, count, *refs):
    chunks = refs[:count]
    (phase_ref, inverse_ref, forward_ref, local_ref, bias_ref, field_ref, cot_ref) = refs[
        count : count + 7
    ]
    grad_ref, sums_ref, rows, mixer, total, outer = refs[count + 7 :]
    step = pl.program_id(0)
    size = chans * GROUP
    here, tile = field_ref.shape[1:]
    lanes = 2 * modes

    @pl.when(step == 0)
    def _():
        inverse_rows(chans, modes, scale, phase_ref[...], chunks, True, rows)
        mixer[...] = channel_map(local_ref, chans, False)
        total[...] = jnp.zeros_like(total)
        outer[...] = jnp.zeros_like(outer)
        sums_ref[...] = jnp.zeros_like(sums_ref)

    mix = mixer[...]
    group = lax.broadcasted_iota(jnp.int32, (size, chans), 0) // GROUP
    pick = group == lax.broadcasted_iota(jnp.int32, (size, chans), 1)
    bias = jnp.sum(jnp.where(pick, bias_ref[...], 0.0), axis=1, keepdims=True)
    both = jnp.zeros((size, size), F32)
    for at in range(0, here, GROUP):
        block = slice(at, at + GROUP)
        mine = rows[at * chans : (at + GROUP) * chans]
        field = field_ref[:, block, :].reshape(size, tile)
        preact = dot(mix, field) + dot(mine, inverse_ref[...]) + bias
        cot = cot_ref[:, block, :].reshape(size, tile)
        grad = cot * gelu_slope(preact.astype(BF16))
        grad_ref[:, block, :] = grad.reshape(chans, GROUP, tile)
        both = both + dot_nt(field, grad)
    outer[...] += both
    total[...] += dot(grad_ref[...].reshape(chans * here, tile), forward_ref[...])

    @pl.when(step == pl.num_programs(0) - 1)
    def _():
        for o in range(chans):
            sums_ref[:, o * lanes : (o + 1) * lanes] = total[o * here : (o + 1) * here].astype(BF16)
        row = lax.broadcasted_iota(jnp.int32, (size, size), 0) % GROUP
        lane = lax.broadcasted_iota(jnp.int32, (size, size), 1) % GROUP
        same = jnp.where(row == lane, outer[...], 0.0).reshape(chans, GROUP, size)
        folded = jnp.sum(same, axis=1)
        wider = lax.broadcasted_iota(jnp.int32, (size, LANES), 0) // GROUP
        gather = wider == lax.broadcasted_iota(jnp.int32, (size, LANES), 1)
        local = jnp.dot(
            folded,
            jnp.where(gather, 1.0, 0.0),
            precision=lax.Precision.HIGHEST,
            preferred_element_type=F32,
        )
        biases = jnp.sum(total[:, :modes].reshape(chans, here, modes), axis=1)[:, :1]
        place = lax.broadcasted_iota(jnp.int32, (chans, LANES), 1)
        line = lax.broadcasted_iota(jnp.int32, (chans, LANES), 0)
        across = jnp.sum(jnp.where(place == chans + line, biases, 0.0), axis=0, keepdims=True)
        small = jnp.where(place < chans, local, jnp.where(line == 0, across, 0.0))
        sums_ref[:chans, chans * lanes :] = to_pieces(small).astype(BF16)


def field_kernel(chans, modes, scale, count, *refs):
    chunks = refs[:count]
    phase_ref, inverse_ref, local_ref, grad_ref, out_ref, rows, mixer = refs[count:]
    size = chans * GROUP
    here, tile = grad_ref.shape[1:]

    @pl.when(pl.program_id(0) == 0)
    def _():
        inverse_rows(chans, modes, scale, phase_ref[...], chunks, False, rows)
        mixer[...] = channel_map(local_ref, chans, True)

    mix = mixer[...]
    for at in range(0, here, GROUP):
        block = slice(at, at + GROUP)
        mine = rows[at * chans : (at + GROUP) * chans]
        value = dot(mix, grad_ref[:, block, :].reshape(size, tile)) + dot(mine, inverse_ref[...])
        out_ref[:, block, :] = value.astype(BF16).reshape(chans, GROUP, tile)


def swap(value, axis, mask):
    size = lax.axis_size(axis)
    return lax.ppermute(value, axis, [(at, at ^ mask) for at in range(size)])


def on_device(fields, cotangent, spectral, local_weight, bias):
    field = fields[0]
    cot = cotangent[0]
    chans, rows_here, width = field.shape
    owned, modes = spectral.shape[3:]
    row_count = lax.axis_size("row")
    map_count = lax.axis_size("dp")
    chips = row_count // 2
    height = rows_here * row_count
    scale = 1.0 / math.sqrt(height * width)
    grad_scale = 1.0 / math.sqrt(map_count * height * width)
    lanes = 2 * modes
    flat = chans * lanes
    size = chans * GROUP
    extra = LANES * max(1, chans // owned)
    assert 2 * chans <= 32
    aligned = owned % GROUP == 0

    me = lax.axis_index("row")
    chip, core = me // 2, me % 2
    inverse_const = column_table(width, modes)
    inverse = jnp.asarray(inverse_const)
    forward = jnp.asarray(np.ascontiguousarray(inverse_const.T))

    near = jnp.arange(chips, dtype=jnp.int32) ^ chip
    inner = jnp.arange(owned, dtype=jnp.int32)
    own_modes = ((2 * near + core)[:, None] * owned + inner[None, :]).reshape(-1)
    far_modes = ((2 * near + 1 - core)[:, None] * owned + inner[None, :]).reshape(-1)
    here = jnp.arange(rows_here, dtype=jnp.int32)
    pair_rows = jnp.concatenate([me * rows_here + here, (me ^ 1) * rows_here + here])
    angle = row_angles(own_modes, pair_rows, height, modes)
    to_modes = jnp.concatenate([jnp.cos(angle), jnp.sin(angle)], axis=0).astype(BF16)
    all_modes = jnp.concatenate([own_modes, far_modes])
    angle = row_angles(all_modes, me * rows_here + here, height, modes).T
    to_rows = jnp.concatenate([jnp.cos(angle), jnp.sin(angle)], axis=0).astype(BF16)


    def blocks(most):
        tile = min(most, width)
        return (
            width // tile,
            pl.BlockSpec((chans, rows_here, tile), lambda i: (0, 0, i)),
            pl.BlockSpec((lanes, tile), lambda i: (0, i)),
            pl.BlockSpec((tile, lanes), lambda i: (i, 0)),
        )

    tiles, block, inverse_block, forward_block = blocks(TILE)
    main_tiles, main_block, main_inverse, main_forward = blocks(MAIN_TILE)

    def rows_step(mine, other, more):
        out_lanes = flat + (extra if more else 0)
        if aligned:
            shapes = [jax.ShapeDtypeStruct((owned, out_lanes), BF16)] * chips
        else:
            shapes = [jax.ShapeDtypeStruct((chips * owned, flat), BF16)]
        kernel = functools.partial(rows_kernel, chans, modes, scale, more and aligned)
        outs = pl.pallas_call(
            kernel,
            name="rows",
            out_shape=shapes,
            compiler_params=room(8),
            cost_estimate=pl.CostEstimate(
                flops=4 * chips * owned * 2 * rows_here * flat,
                transcendentals=0,
                bytes_accessed=6 * rows_here * flat,
            ),
        )(mine, other, to_modes)
        if aligned:
            return outs
        pieces = jnp.split(outs[0], chips, axis=0)
        if more:
            packed = small_sum(mine[:chans, flat:], other[:chans, flat:])
            packed = packed.reshape(chans // owned, owned, LANES).transpose(1, 0, 2)
            packed = packed.reshape(owned, extra)
            pieces = [jnp.concatenate([piece, packed], axis=1) for piece in pieces]
        return pieces

    def small_sum(mine, other):
        def kernel(a, b, out):
            total = from_pieces(a[...].astype(F32)) + from_pieces(b[...].astype(F32))
            out[...] = to_pieces(keep_low(total)).astype(BF16)

        return pl.pallas_call(
            kernel, name="small", out_shape=jax.ShapeDtypeStruct((chans, LANES), BF16)
        )(mine, other)

    def across_chips(pieces):
        came = [pieces[0]]
        for d in range(1, chips):
            came.append(swap(pieces[d], "row", 2 * d))
        return came

    def gather(piece):
        same = across_chips([piece] * chips)
        chunks = same + [swap(part, "row", 1) for part in same]
        return chunks if aligned else [jnp.concatenate(chunks, axis=0)]

    coeffs = pl.pallas_call(
        columns_kernel,
        name="columns",
        grid=(tiles,),
        in_specs=[block, forward_block],
        out_specs=whole((rows_here, flat)),
        out_shape=jax.ShapeDtypeStruct((rows_here, flat), BF16),
        scratch_shapes=[pltpu.VMEM((chans * rows_here, lanes), F32)],
        compiler_params=room(12),
    )(streamed(field), streamed(forward))
    chunks = across_chips(rows_step(coeffs, swap(coeffs, "row", 1), False))

    mixed, spectrum = pl.pallas_call(
        functools.partial(mix_kernel, chans, modes, chips),
        name="mix",
        out_shape=[jax.ShapeDtypeStruct((owned, flat), BF16)] * 2,
        scratch_shapes=[pltpu.VMEM((2 * chans, owned, modes), F32)],
        compiler_params=room(10),
    )(spectral, *chunks)
    mixed = gather(mixed)
    spectra = [spectrum] + [swap(spectrum, "dp", d) for d in range(1, map_count)]

    chunk_specs = [whole(part.shape) for part in mixed]
    main = pl.pallas_call(
        functools.partial(main_kernel, chans, modes, scale, len(mixed)),
        name="main",
        grid=(main_tiles,),
        in_specs=chunk_specs
        + [
            whole(to_rows.shape),
            main_inverse,
            main_forward,
            whole((chans, chans)),
            whole((1, chans)),
            main_block,
            main_block,
        ],
        out_specs=[main_block, whole((rows_here, flat + LANES))],
        out_shape=[
            pltpu.HBM(field.shape, BF16),
            jax.ShapeDtypeStruct((rows_here, flat + LANES), BF16),
        ],
        scratch_shapes=[
            pltpu.VMEM((chans * rows_here, lanes), BF16),
            pltpu.VMEM((size, size), BF16),
            pltpu.VMEM((chans * rows_here, lanes), F32),
            pltpu.VMEM((size, size), F32),
        ],
        compiler_params=room(28),
    )
    grad_pre, grad_coeffs = main(
        *mixed, to_rows, streamed(inverse), streamed(forward), local_weight, bias[None], streamed(field), streamed(cot)
    )

    chunks = across_chips(rows_step(grad_coeffs, swap(grad_coeffs, "row", 1), True))
    part_lanes = chans // map_count * lanes
    outs = pl.pallas_call(
        functools.partial(back_kernel, chans, modes, chips, map_count),
        name="back",
        in_specs=[pl.BlockSpec(memory_space=pltpu.SMEM)]
        + [pl.BlockSpec(memory_space=pltpu.VMEM)] * (1 + chips),
        out_shape=[jax.ShapeDtypeStruct((owned, flat), BF16)]
        + [jax.ShapeDtypeStruct((owned, part_lanes + extra), BF16)] * map_count,
        scratch_shapes=[
            pltpu.VMEM((2 * chans, owned, modes), F32),
            pltpu.VMEM((owned, flat), BF16),
        ],
        compiler_params=room(10),
    )(lax.axis_index("dp").astype(jnp.int32)[None], spectral, *chunks)
    freq_grad = gather(outs[0])
    slices = [outs[1]] + [swap(outs[1 + d], "dp", d) for d in range(1, map_count)]

    steps = 1
    spectral_grad, local_grad, bias_grad = pl.pallas_call(
        functools.partial(weight_kernel, chans, modes, map_count, grad_scale),
        name="weights",
        grid=(steps,),
        in_specs=[pl.BlockSpec((owned, flat // steps), lambda i: (0, i))] * map_count
        + [whole(slices[0].shape)] * map_count,
        out_specs=[
            pl.BlockSpec(
                (2, chans // steps, chans // map_count, owned, modes), lambda i: (0, i, 0, 0, 0)
            ),
            whole((chans, chans)),
            whole((1, chans)),
        ],
        out_shape=[
            pltpu.HBM((2, chans, chans // map_count, owned, modes), F32),
            jax.ShapeDtypeStruct((chans, chans), F32),
            jax.ShapeDtypeStruct((1, chans), F32),
        ],
        compiler_params=room(12),
    )(*spectra, *slices)

    final = pl.pallas_call(
        functools.partial(field_kernel, chans, modes, scale, len(freq_grad)),
        name="field",
        grid=(tiles,),
        in_specs=[whole(part.shape) for part in freq_grad]
        + [whole(to_rows.shape), inverse_block, whole((chans, chans)), block],
        out_specs=block,
        out_shape=pltpu.HBM(field.shape, BF16),
        scratch_shapes=[
            pltpu.VMEM((chans * rows_here, lanes), BF16),
            pltpu.VMEM((size, size), BF16),
        ],
        compiler_params=room(20),
    )
    field_grad = final(
        *freq_grad, to_rows, streamed(inverse), local_weight, streamed(grad_pre)
    )

    return (field_grad[None], spectral_grad, local_grad, bias_grad[0])


def solution(mesh):
    return jax.shard_map(
        on_device,
        mesh=mesh,
        in_specs=(
            P("dp", None, "row", None),
            P("dp", None, "row", None),
            P(None, None, None, "row", None),
            P(),
            P(),
        ),
        out_specs=(P("dp", None, "row", None), P(None, None, "dp", "row", None), P(), P()),
        check_vma=False,
    )
```

```python
import functools
import math

import jax
import jax.numpy as jnp
import numpy as np
from jax import lax
from jax.experimental import pallas as pl
from jax.experimental.pallas import tpu as pltpu
from jax.sharding import PartitionSpec as P


BF16 = jnp.bfloat16
F32 = jnp.float32
LANES = 128
TILE = 1024
MAIN_TILE = 512
GROUP = 16


def column_table(width, modes):
    turns = np.arange(modes)[:, None] * np.arange(width)[None, :] % width
    angle = np.float32(2.0 * math.pi / width) * turns.astype(np.float32)
    table = np.concatenate([np.cos(angle), -np.sin(angle)], axis=0)
    return table.astype(BF16)


def row_angles(mode, place, height, modes):
    freq = (mode - modes // 2) % height
    turns = freq[:, None] * place[None, :] % height
    return 2.0 * math.pi / height * turns.astype(F32)


def dot(left, right):
    return jnp.dot(left, right, preferred_element_type=F32)


def dot_nt(left, right):
    return lax.dot_general(left, right, (((1,), (1,)), ((), ())), preferred_element_type=F32)


def tree(parts):
    parts = list(parts)
    while len(parts) > 1:
        parts = [parts[at] + parts[at + 1] for at in range(0, len(parts), 2)]
    return parts[0]


def whole(shape):
    return pl.BlockSpec(shape, lambda *_: (0,) * len(shape))


def room(mebibytes):
    return pltpu.CompilerParams(vmem_limit_bytes=mebibytes << 20)


def streamed(value):
    return pltpu.with_memory_space_constraint(value, pltpu.HBM)


def to_pieces(value):
    first = value.astype(BF16).astype(F32)
    rest = value - first
    second = rest.astype(BF16).astype(F32)
    third = rest - second
    return first + pltpu.roll(second, 32, 1) + pltpu.roll(third, 64, 1)


def from_pieces(packed):
    back = LANES
    return packed + pltpu.roll(packed, back - 32, 1) + pltpu.roll(packed, back - 64, 1)


def columns_kernel(field_ref, table_ref, out_ref, total):
    chans, rows, tile = field_ref.shape
    lanes = table_ref.shape[1]
    step = pl.program_id(0)
    part = dot(field_ref[...].reshape(chans * rows, tile), table_ref[...])

    @pl.when(step == 0)
    def _():
        total[...] = part

    @pl.when(step > 0)
    def _():
        total[...] += part

    @pl.when(step == pl.num_programs(0) - 1)
    def _():
        for c in range(chans):
            out_ref[:, c * lanes : (c + 1) * lanes] = total[c * rows : (c + 1) * rows].astype(BF16)


def rows_kernel(chans, modes, scale, extra, mine_ref, other_ref, phase_ref, *outs):
    half = phase_ref.shape[0] // 2
    lanes = 2 * modes
    phase = phase_ref[...]
    for c in range(chans):
        at = slice(c * lanes, (c + 1) * lanes)
        both = jnp.concatenate([mine_ref[:, at], other_ref[:, at]], axis=0)
        part = dot(phase, both)
        real = part[:half, :modes] + part[half:, modes:]
        imag = part[:half, modes:] - part[half:, :modes]
        full = (scale * jnp.concatenate([real, imag], axis=1)).astype(BF16)
        size = half // len(outs)
        for d, out in enumerate(outs):
            out[:, at] = full[d * size : (d + 1) * size]
    if extra:
        top = chans * lanes
        rows = chans
        total = from_pieces(mine_ref[:rows, top:].astype(F32)) + from_pieces(
            other_ref[:rows, top:].astype(F32)
        )
        packed = to_pieces(keep_low(total)).astype(BF16)
        for out in outs:
            put_pieces(out, packed, top, rows)


def keep_low(value):
    lane = lax.broadcasted_iota(jnp.int32, value.shape, 1)
    return jnp.where(lane < 32, value, 0.0)


def put_pieces(out, packed, top, rows):
    size = out.shape[0]
    if size >= rows:
        out[:rows, top : top + LANES] = packed
        if size > rows:
            out[rows:, top : top + LANES] = jnp.zeros((size - rows, LANES), packed.dtype)
        return
    for e in range(rows // size):
        out[:, top + e * LANES : top + (e + 1) * LANES] = packed[e * size : (e + 1) * size]


def get_pieces(ref, top, rows):
    size = ref.shape[0]
    if size >= rows:
        return ref[:rows, top : top + LANES].astype(F32)
    return jnp.concatenate(
        [
            ref[:, top + e * LANES : top + (e + 1) * LANES].astype(F32)
            for e in range(rows // size)
        ],
        axis=0,
    )


def mix_kernel(chans, modes, count, weight_ref, *refs):
    chunks = refs[:count]
    mixed_ref, spectrum_ref, sums = refs[count:]
    lanes = 2 * modes
    for c in range(2 * chans):
        at = slice(c * modes, (c + 1) * modes)
        value = tree([chunk[:, at].astype(F32) for chunk in chunks])
        sums[c] = value
        spectrum_ref[:, at] = value.astype(BF16)

    for o in range(chans):
        real = imag = None
        for c in range(chans):
            wr = weight_ref[0, c, o].astype(F32)
            wi = weight_ref[1, c, o].astype(F32)
            fr = sums[2 * c]
            fi = sums[2 * c + 1]
            a = wr * fr - wi * fi
            b = wr * fi + wi * fr
            real = a if real is None else real + a
            imag = b if imag is None else imag + b
        mixed_ref[:, o * lanes : o * lanes + modes] = real.astype(BF16)
        mixed_ref[:, o * lanes + modes : (o + 1) * lanes] = imag.astype(BF16)


def back_kernel(chans, modes, count, maps, where_ref, weight_ref, *refs):
    chunks = refs[:count]
    back_ref = refs[count]
    slices = refs[count + 1 : count + 1 + maps]
    sums, gathered = refs[count + 1 + maps :]
    lanes = 2 * modes
    shape = (chunks[0].shape[0], modes)
    doubling = jnp.where(lax.broadcasted_iota(jnp.int32, shape, 1) == 0, 1.0, 2.0)
    for c in range(2 * chans):
        at = slice(c * modes, (c + 1) * modes)
        value = tree([chunk[:, at].astype(F32) for chunk in chunks]) * doubling
        sums[c] = value
        gathered[:, at] = value.astype(BF16)

    for c in range(chans):
        real = imag = None
        for o in range(chans):
            wr = weight_ref[0, c, o].astype(F32)
            wi = weight_ref[1, c, o].astype(F32)
            gr = sums[2 * o]
            gi = sums[2 * o + 1]
            a = wr * gr + wi * gi
            b = wr * gi - wi * gr
            real = a if real is None else real + a
            imag = b if imag is None else imag + b
        back_ref[:, c * lanes : c * lanes + modes] = real.astype(BF16)
        back_ref[:, c * lanes + modes : (c + 1) * lanes] = imag.astype(BF16)

    top = chans * lanes
    total = tree([from_pieces(get_pieces(chunk, top, chans)) for chunk in chunks])
    packed = to_pieces(keep_low(total)).astype(BF16)
    span = chans // maps * lanes
    for d, out in enumerate(slices):
        first = pl.multiple_of((where_ref[0] ^ d) * span, LANES)
        out[:, :span] = gathered[:, pl.ds(first, span)]
        put_pieces(out, packed, span, chans)


def weight_kernel(chans, modes, maps, scale, *refs):
    spectra = refs[:maps]
    slices = refs[maps : 2 * maps]
    grad_ref, local_ref, bias_ref = refs[2 * maps :]
    lanes = 2 * modes
    part = chans // maps
    for o in range(part):
        at = o * lanes
        grads = [
            (s[:, at : at + modes].astype(F32), s[:, at + modes : at + lanes].astype(F32))
            for s in slices
        ]
        for c in range(grad_ref.shape[1]):
            at = c * lanes
            real = []
            imag = []
            for spectrum, (gr, gi) in zip(spectra, grads):
                fr = spectrum[:, at : at + modes].astype(F32)
                fi = spectrum[:, at + modes : at + lanes].astype(F32)
                real.append(gr * fr + gi * fi)
                imag.append(gi * fr - gr * fi)
            grad_ref[0, c, o] = tree(real)
            grad_ref[1, c, o] = tree(imag)

    @pl.when(pl.program_id(0) == 0)
    def _():
        small = [from_pieces(get_pieces(s, part * lanes, chans)) for s in slices]
        small = scale * tree(small)
        local_ref[...] = small[:, :chans]
        bias_ref[...] = pltpu.roll(small, LANES - chans, 1)[:1, :chans]


def channel_map(local_ref, chans, back):
    size = chans * GROUP
    pick = (
        lax.broadcasted_iota(jnp.int32, (size, chans), 0) // GROUP
        == lax.broadcasted_iota(jnp.int32, (size, chans), 1)
    )
    pick = jnp.where(pick, 1.0, 0.0).astype(BF16)
    local = local_ref[...]
    if back:
        wide = dot(pick, local).astype(BF16)
    else:
        wide = lax.dot_general(
            pick, local, (((1,), (1,)), ((), ())), preferred_element_type=F32
        ).astype(BF16)
    full = dot_nt(wide, pick)
    row = lax.broadcasted_iota(jnp.int32, (size, size), 0) % GROUP
    lane = lax.broadcasted_iota(jnp.int32, (size, size), 1) % GROUP
    return jnp.where(row == lane, full, 0.0).astype(BF16)


def inverse_rows(chans, modes, scale, phase, chunks, doubled, out):
    lanes = 2 * modes
    half = phase.shape[0] // 2
    factor = jnp.full((1, modes), scale, F32)
    if doubled:
        first = lax.broadcasted_iota(jnp.int32, (1, modes), 1) == 0
        factor = jnp.where(first, scale, 2.0 * scale)
    for o in range(chans):
        at = slice(o * lanes, (o + 1) * lanes)
        part = dot(phase, jnp.concatenate([chunk[:, at] for chunk in chunks], axis=0))
        real = ((part[:half, :modes] - part[half:, modes:]) * factor).astype(BF16)
        imag = ((part[:half, modes:] + part[half:, :modes]) * factor).astype(BF16)
        for at in range(0, half, GROUP):
            first = at * chans + o * GROUP
            out[first : first + GROUP, :modes] = real[at : at + GROUP]
            out[first : first + GROUP, modes:] = imag[at : at + GROUP]


SLOPE = math.sqrt(2.0 / math.pi)
CUBIC = 0.044715


def gelu_slope(x):
    kind = x.dtype.type
    square = x * x
    inner = x * (kind(SLOPE) + kind(SLOPE * CUBIC) * square)
    outer = x * (kind(0.5 * SLOPE) + kind(1.5 * SLOPE * CUBIC) * square)
    t = jnp.tanh(inner)
    return (kind(1.0) + t) * (kind(0.5) + (kind(1.0) - t) * outer)


def main_kernel(chans, modes, scale, count, *refs):
    chunks = refs[:count]
    (phase_ref, inverse_ref, forward_ref, local_ref, bias_ref, field_ref, cot_ref) = refs[
        count : count + 7
    ]
    grad_ref, sums_ref, rows, mixer, total, outer = refs[count + 7 :]
    step = pl.program_id(0)
    size = chans * GROUP
    here, tile = field_ref.shape[1:]
    lanes = 2 * modes

    @pl.when(step == 0)
    def _():
        inverse_rows(chans, modes, scale, phase_ref[...], chunks, True, rows)
        mixer[...] = channel_map(local_ref, chans, False)
        total[...] = jnp.zeros_like(total)
        outer[...] = jnp.zeros_like(outer)
        sums_ref[:, chans * lanes :] = jnp.zeros((here, sums_ref.shape[1] - chans * lanes), BF16)

    mix = mixer[...]
    group = lax.broadcasted_iota(jnp.int32, (size, chans), 0) // GROUP
    pick = group == lax.broadcasted_iota(jnp.int32, (size, chans), 1)
    bias = jnp.sum(jnp.where(pick, bias_ref[...], 0.0), axis=1, keepdims=True)
    both = jnp.zeros((size, size), F32)
    for at in range(0, here, GROUP):
        block = slice(at, at + GROUP)
        mine = rows[at * chans : (at + GROUP) * chans]
        field = field_ref[:, block, :].reshape(size, tile)
        preact = dot(mix, field) + dot(mine, inverse_ref[...]) + bias
        cot = cot_ref[:, block, :].reshape(size, tile)
        grad = cot * gelu_slope(preact.astype(BF16))
        grad_ref[:, block, :] = grad.reshape(chans, GROUP, tile)
    for at in range(0, here, GROUP):
        block = slice(at, at + GROUP)
        field = field_ref[:, block, :].reshape(size, tile)
        both = both + dot_nt(field, grad_ref[:, block, :].reshape(size, tile))
    outer[...] += both
    total[...] += dot(grad_ref[...].reshape(chans * here, tile), forward_ref[...])

    @pl.when(step == pl.num_programs(0) - 1)
    def _():
        for o in range(chans):
            sums_ref[:, o * lanes : (o + 1) * lanes] = total[o * here : (o + 1) * here].astype(BF16)
        row = lax.broadcasted_iota(jnp.int32, (size, size), 0) % GROUP
        lane = lax.broadcasted_iota(jnp.int32, (size, size), 1) % GROUP
        same = jnp.where(row == lane, outer[...], 0.0).reshape(chans, GROUP, size)
        folded = jnp.sum(same, axis=1)
        wider = lax.broadcasted_iota(jnp.int32, (size, LANES), 0) // GROUP
        gather = wider == lax.broadcasted_iota(jnp.int32, (size, LANES), 1)
        local = jnp.dot(
            folded,
            jnp.where(gather, 1.0, 0.0),
            precision=lax.Precision.HIGHEST,
            preferred_element_type=F32,
        )
        biases = jnp.sum(total[:, :modes].reshape(chans, here, modes), axis=1)[:, :1]
        place = lax.broadcasted_iota(jnp.int32, (chans, LANES), 1)
        line = lax.broadcasted_iota(jnp.int32, (chans, LANES), 0)
        across = jnp.sum(jnp.where(place == chans + line, biases, 0.0), axis=0, keepdims=True)
        small = jnp.where(place < chans, local, jnp.where(line == 0, across, 0.0))
        sums_ref[:chans, chans * lanes :] = to_pieces(small).astype(BF16)


def field_kernel(chans, modes, scale, count, *refs):
    chunks = refs[:count]
    phase_ref, inverse_ref, local_ref, grad_ref, out_ref, rows, mixer, wide = refs[count:]
    size = chans * GROUP
    here, tile = grad_ref.shape[1:]

    @pl.when(pl.program_id(0) == 0)
    def _():
        inverse_rows(chans, modes, scale, phase_ref[...], chunks, False, rows)
        mixer[...] = channel_map(local_ref, chans, True)

    mix = mixer[...]
    wide[...] = dot(rows[...], inverse_ref[...])
    for at in range(0, here, GROUP):
        block = slice(at, at + GROUP)
        value = dot(mix, grad_ref[:, block, :].reshape(size, tile))
        value = value + wide[at * chans : (at + GROUP) * chans]
        out_ref[:, block, :] = value.astype(BF16).reshape(chans, GROUP, tile)


def swap(value, axis, mask):
    size = lax.axis_size(axis)
    return lax.ppermute(value, axis, [(at, at ^ mask) for at in range(size)])


def on_device(fields, cotangent, spectral, local_weight, bias):
    field = fields[0]
    cot = cotangent[0]
    chans, rows_here, width = field.shape
    owned, modes = spectral.shape[3:]
    row_count = lax.axis_size("row")
    map_count = lax.axis_size("dp")
    chips = row_count // 2
    height = rows_here * row_count
    scale = 1.0 / math.sqrt(height * width)
    grad_scale = 1.0 / math.sqrt(map_count * height * width)
    lanes = 2 * modes
    flat = chans * lanes
    size = chans * GROUP
    extra = LANES * max(1, chans // owned)
    assert 2 * chans <= 32
    aligned = owned % GROUP == 0

    me = lax.axis_index("row")
    chip, core = me // 2, me % 2
    inverse_const = column_table(width, modes)
    inverse = jnp.asarray(inverse_const)
    forward = jnp.asarray(np.ascontiguousarray(inverse_const.T))

    near = jnp.arange(chips, dtype=jnp.int32) ^ chip
    inner = jnp.arange(owned, dtype=jnp.int32)
    own_modes = ((2 * near + core)[:, None] * owned + inner[None, :]).reshape(-1)
    far_modes = ((2 * near + 1 - core)[:, None] * owned + inner[None, :]).reshape(-1)
    here = jnp.arange(rows_here, dtype=jnp.int32)
    pair_rows = jnp.concatenate([me * rows_here + here, (me ^ 1) * rows_here + here])
    angle = row_angles(own_modes, pair_rows, height, modes)
    to_modes = jnp.concatenate([jnp.cos(angle), jnp.sin(angle)], axis=0).astype(BF16)
    all_modes = jnp.concatenate([own_modes, far_modes])
    angle = row_angles(all_modes, me * rows_here + here, height, modes).T
    to_rows = jnp.concatenate([jnp.cos(angle), jnp.sin(angle)], axis=0).astype(BF16)


    def blocks(most):
        tile = min(most, width)
        return (
            width // tile,
            pl.BlockSpec((chans, rows_here, tile), lambda i: (0, 0, i)),
            pl.BlockSpec((lanes, tile), lambda i: (0, i)),
            pl.BlockSpec((tile, lanes), lambda i: (i, 0)),
        )

    tiles, block, inverse_block, forward_block = blocks(TILE)
    main_tiles, main_block, main_inverse, main_forward = blocks(MAIN_TILE)

    def rows_step(mine, other, more):
        out_lanes = flat + (extra if more else 0)
        if aligned:
            shapes = [jax.ShapeDtypeStruct((owned, out_lanes), BF16)] * chips
        else:
            shapes = [jax.ShapeDtypeStruct((chips * owned, flat), BF16)]
        kernel = functools.partial(rows_kernel, chans, modes, scale, more and aligned)
        outs = pl.pallas_call(
            kernel,
            name="rows",
            out_shape=shapes,
            compiler_params=room(8),
            cost_estimate=pl.CostEstimate(
                flops=4 * chips * owned * 2 * rows_here * flat,
                transcendentals=0,
                bytes_accessed=6 * rows_here * flat,
            ),
        )(mine, other, to_modes)
        if aligned:
            return outs
        pieces = jnp.split(outs[0], chips, axis=0)
        if more:
            packed = small_sum(mine[:chans, flat:], other[:chans, flat:])
            packed = packed.reshape(chans // owned, owned, LANES).transpose(1, 0, 2)
            packed = packed.reshape(owned, extra)
            pieces = [jnp.concatenate([piece, packed], axis=1) for piece in pieces]
        return pieces

    def small_sum(mine, other):
        def kernel(a, b, out):
            total = from_pieces(a[...].astype(F32)) + from_pieces(b[...].astype(F32))
            out[...] = to_pieces(keep_low(total)).astype(BF16)

        return pl.pallas_call(
            kernel, name="small", out_shape=jax.ShapeDtypeStruct((chans, LANES), BF16)
        )(mine, other)

    def across_chips(pieces):
        came = [pieces[0]]
        for d in range(1, chips):
            came.append(swap(pieces[d], "row", 2 * d))
        return came

    def gather(piece):
        same = across_chips([piece] * chips)
        chunks = same + [swap(part, "row", 1) for part in same]
        return chunks if aligned else [jnp.concatenate(chunks, axis=0)]

    coeffs = pl.pallas_call(
        columns_kernel,
        name="columns",
        grid=(tiles,),
        in_specs=[block, forward_block],
        out_specs=whole((rows_here, flat)),
        out_shape=jax.ShapeDtypeStruct((rows_here, flat), BF16),
        scratch_shapes=[pltpu.VMEM((chans * rows_here, lanes), F32)],
        compiler_params=room(12),
    )(streamed(field), streamed(forward))
    chunks = across_chips(rows_step(coeffs, swap(coeffs, "row", 1), False))

    mixed, spectrum = pl.pallas_call(
        functools.partial(mix_kernel, chans, modes, chips),
        name="mix",
        out_shape=[jax.ShapeDtypeStruct((owned, flat), BF16)] * 2,
        scratch_shapes=[pltpu.VMEM((2 * chans, owned, modes), F32)],
        compiler_params=room(10),
    )(spectral, *chunks)
    mixed = gather(mixed)
    spectra = [spectrum] + [swap(spectrum, "dp", d) for d in range(1, map_count)]

    chunk_specs = [whole(part.shape) for part in mixed]
    main = pl.pallas_call(
        functools.partial(main_kernel, chans, modes, scale, len(mixed)),
        name="main",
        grid=(main_tiles,),
        in_specs=chunk_specs
        + [
            whole(to_rows.shape),
            main_inverse,
            main_forward,
            whole((chans, chans)),
            whole((1, chans)),
            main_block,
            main_block,
        ],
        out_specs=[main_block, whole((rows_here, flat + LANES))],
        out_shape=[
            pltpu.HBM(field.shape, BF16),
            jax.ShapeDtypeStruct((rows_here, flat + LANES), BF16),
        ],
        scratch_shapes=[
            pltpu.VMEM((chans * rows_here, lanes), BF16),
            pltpu.VMEM((size, size), BF16),
            pltpu.VMEM((chans * rows_here, lanes), F32),
            pltpu.VMEM((size, size), F32),
        ],
        compiler_params=room(28),
    )
    grad_pre, grad_coeffs = main(
        *mixed, to_rows, streamed(inverse), streamed(forward), local_weight, bias[None], streamed(field), streamed(cot)
    )

    chunks = across_chips(rows_step(grad_coeffs, swap(grad_coeffs, "row", 1), True))
    part_lanes = chans // map_count * lanes
    outs = pl.pallas_call(
        functools.partial(back_kernel, chans, modes, chips, map_count),
        name="back",
        in_specs=[pl.BlockSpec(memory_space=pltpu.SMEM)]
        + [pl.BlockSpec(memory_space=pltpu.VMEM)] * (1 + chips),
        out_shape=[jax.ShapeDtypeStruct((owned, flat), BF16)]
        + [jax.ShapeDtypeStruct((owned, part_lanes + extra), BF16)] * map_count,
        scratch_shapes=[
            pltpu.VMEM((2 * chans, owned, modes), F32),
            pltpu.VMEM((owned, flat), BF16),
        ],
        compiler_params=room(10),
    )(lax.axis_index("dp").astype(jnp.int32)[None], spectral, *chunks)
    freq_grad = gather(outs[0])
    slices = [outs[1]] + [swap(outs[1 + d], "dp", d) for d in range(1, map_count)]

    steps = 1
    spectral_grad, local_grad, bias_grad = pl.pallas_call(
        functools.partial(weight_kernel, chans, modes, map_count, grad_scale),
        name="weights",
        grid=(steps,),
        in_specs=[pl.BlockSpec((owned, flat // steps), lambda i: (0, i))] * map_count
        + [whole(slices[0].shape)] * map_count,
        out_specs=[
            pl.BlockSpec(
                (2, chans // steps, chans // map_count, owned, modes), lambda i: (0, i, 0, 0, 0)
            ),
            whole((chans, chans)),
            whole((1, chans)),
        ],
        out_shape=[
            pltpu.HBM((2, chans, chans // map_count, owned, modes), F32),
            jax.ShapeDtypeStruct((chans, chans), F32),
            jax.ShapeDtypeStruct((1, chans), F32),
        ],
        compiler_params=room(12),
    )(*spectra, *slices)

    final = pl.pallas_call(
        functools.partial(field_kernel, chans, modes, scale, len(freq_grad)),
        name="field",
        grid=(tiles,),
        in_specs=[whole(part.shape) for part in freq_grad]
        + [whole(to_rows.shape), inverse_block, whole((chans, chans)), block],
        out_specs=block,
        out_shape=pltpu.HBM(field.shape, BF16),
        scratch_shapes=[
            pltpu.VMEM((chans * rows_here, lanes), BF16),
            pltpu.VMEM((size, size), BF16),
            pltpu.VMEM((chans * rows_here, block.block_shape[2]), F32),
        ],
        compiler_params=room(20),
    )
    field_grad = final(
        *freq_grad, to_rows, streamed(inverse), local_weight, streamed(grad_pre)
    )

    return (field_grad[None], spectral_grad, local_grad, bias_grad[0])


def solution(mesh):
    return jax.shard_map(
        on_device,
        mesh=mesh,
        in_specs=(
            P("dp", None, "row", None),
            P("dp", None, "row", None),
            P(None, None, None, "row", None),
            P(),
            P(),
        ),
        out_specs=(P("dp", None, "row", None), P(None, None, "dp", "row", None), P(), P()),
        check_vma=False,
    )
```
